16 devices in a mesh: dp: 4 (over z, y), tp: 4 (over x, core).
Axes of the slice: x: 2, y: 2, z: 2, core: 2. Of those that a mesh axis runs over, the one named last changes fastest.
Arguments:
- x_in: bfloat16 [32, 2048, 1024], P('dp'), parts along dimension 0
- start_pos: int32 [32], P('dp'), parts along dimension 0
- kv_state: float32 [32, 4, 256, 512], P('dp', 'tp'), parts along dimension 0
- ln1_gain: float32 [1024], replicated
- ln1_bias: float32 [1024], replicated
- w_q: bfloat16 [1024, 1024], P(None, 'tp')
- w_k: bfloat16 [1024, 1024], P(None, 'tp')
- w_v: bfloat16 [1024, 2048], P(None, 'tp')
- w_g: bfloat16 [1024, 2048], P(None, 'tp')
- w_o: bfloat16 [2048, 1024], P('tp')
- ln2_gain: float32 [1024], replicated
- ln2_bias: float32 [1024], replicated
- w_up: bfloat16 [1024, 2048], P(None, 'tp')
- w_down: bfloat16 [2048, 1024], P('tp')
Outputs:
- output 1: bfloat16 [32, 2048, 1024], P('dp'), parts along dimension 0
- output 2: float32 [32, 4, 256, 512], P('dp', 'tp'), parts along dimension 0
There are 4 independent parts. The reference program is written for one: setup_inputs(seed, part) draws one part's arguments, and reference() takes and returns one part's arrays. A program takes and returns all parts, laid end to end along the dimension named above; an argument that names none is the same for every part.
All inputs are finite; a program needn't handle non-finite values.
Results may differ from the reference program's by a relative error of at most 0.0132695.
Values are sent between devices in bfloat16 or wider.
A program may use at most 1 GiB of HBM per device.

```python
import jax
import jax.numpy as jnp
from jax import lax

BATCH_SEQS = 8
CHUNK_LEN = 2048
D_MODEL = 1024
NUM_HEADS = 4
FFN_DIM = 2048
POS_LIMIT = 4096

KEY_DIM = D_MODEL // NUM_HEADS
VAL_DIM = 2 * KEY_DIM
HALF_DIM = KEY_DIM // 2
NORM_EPS = 1e-5
GROUP_EPS = 1e-6
ROPE_BASE = 10000.0


def head_log_decay():
    head_ids = jnp.arange(NUM_HEADS).astype(jnp.float32)
    return jnp.log1p(-jnp.exp2(-5.0 - head_ids))


def setup_inputs(seed: int = 0, part: int = 0) -> dict:
    base_key = jax.random.key(seed)
    weight_keys = jax.random.split(base_key, 12)
    part_keys = jax.random.split(jax.random.fold_in(weight_keys[11], part), 3)

    def normal_weight(key_index, arr_shape, fan_in):
        raw_draw = jax.random.normal(weight_keys[key_index], arr_shape, jnp.float32)
        return (raw_draw * fan_in ** -0.5).astype(jnp.bfloat16)

    x_in = jax.random.normal(part_keys[0], (BATCH_SEQS, CHUNK_LEN, D_MODEL), jnp.float32).astype(jnp.bfloat16)
    start_pos = jax.random.randint(part_keys[1], (BATCH_SEQS,), 64, POS_LIMIT, dtype=jnp.int32)
    log_gamma = head_log_decay()
    decayed_var = jnp.expm1(2.0 * start_pos.astype(jnp.float32)[:, None] * log_gamma[None, :]) / jnp.expm1(2.0 * log_gamma)[None, :]
    state_draw = jax.random.normal(part_keys[2], (BATCH_SEQS, NUM_HEADS, KEY_DIM, VAL_DIM), jnp.float32)
    kv_state = state_draw * jnp.sqrt(decayed_var / KEY_DIM)[:, :, None, None]
    return {
        'x_in': x_in,
        'start_pos': start_pos,
        'kv_state': kv_state,
        'ln1_gain': 1.0 + 0.3 * jax.random.normal(weight_keys[0], (D_MODEL,), jnp.float32),
        'ln1_bias': 0.3 * jax.random.normal(weight_keys[1], (D_MODEL,), jnp.float32),
        'w_q': normal_weight(2, (D_MODEL, D_MODEL), D_MODEL),
        'w_k': normal_weight(3, (D_MODEL, D_MODEL), D_MODEL),
        'w_v': normal_weight(4, (D_MODEL, 2 * D_MODEL), D_MODEL),
        'w_g': normal_weight(5, (D_MODEL, 2 * D_MODEL), D_MODEL),
        'w_o': normal_weight(6, (2 * D_MODEL, D_MODEL), 2 * D_MODEL),
        'ln2_gain': 1.0 + 0.3 * jax.random.normal(weight_keys[7], (D_MODEL,), jnp.float32),
        'ln2_bias': 0.3 * jax.random.normal(weight_keys[8], (D_MODEL,), jnp.float32),
        'w_up': normal_weight(9, (D_MODEL, FFN_DIM), D_MODEL),
        'w_down': normal_weight(10, (FFN_DIM, D_MODEL), FFN_DIM),
    }


def layer_norm(x_f32, norm_gain, norm_bias):
    row_mean = jnp.mean(x_f32, axis=-1, keepdims=True)
    centered = x_f32 - row_mean
    variance = jnp.mean(centered * centered, axis=-1, keepdims=True)
    return centered * lax.rsqrt(variance + NORM_EPS) * norm_gain + norm_bias


def rotate_half(head_vecs, cos_t, sin_t):
    first_half = head_vecs[..., :HALF_DIM]
    second_half = head_vecs[..., HALF_DIM:]
    return jnp.concatenate([first_half * cos_t - second_half * sin_t, second_half * cos_t + first_half * sin_t], axis=-1)


def reference(x_in, start_pos, kv_state, ln1_gain, ln1_bias, w_q, w_k, w_v, w_g, w_o, ln2_gain, ln2_bias, w_up, w_down):
    log_gamma = head_log_decay()
    step_ids = jnp.arange(CHUNK_LEN)
    step_gap = step_ids[:, None] - step_ids[None, :]
    inner_decay = jnp.where(step_gap[None] >= 0, jnp.exp(jnp.maximum(step_gap, 0).astype(jnp.float32)[None] * log_gamma[:, None, None]), 0.0)
    query_decay = jnp.exp((step_ids + 1).astype(jnp.float32)[:, None] * log_gamma[None, :])
    key_decay = jnp.exp((CHUNK_LEN - 1 - step_ids).astype(jnp.float32)[:, None] * log_gamma[None, :])
    state_decay = jnp.exp(CHUNK_LEN * log_gamma)
    inv_freq = jnp.power(ROPE_BASE, -jnp.arange(HALF_DIM).astype(jnp.float32) / HALF_DIM)

    def one_sequence(packed):
        tokens, first_pos, old_state = packed
        x_f32 = tokens.astype(jnp.float32)
        h_one = layer_norm(x_f32, ln1_gain, ln1_bias).astype(jnp.bfloat16)
        angles = (first_pos + step_ids).astype(jnp.float32)[:, None] * inv_freq[None, :]
        cos_t = jnp.cos(angles)[:, None, :]
        sin_t = jnp.sin(angles)[:, None, :]
        q_raw = jnp.dot(h_one, w_q, preferred_element_type=jnp.float32).reshape(CHUNK_LEN, NUM_HEADS, KEY_DIM)
        k_raw = jnp.dot(h_one, w_k, preferred_element_type=jnp.float32).reshape(CHUNK_LEN, NUM_HEADS, KEY_DIM)
        queries = rotate_half(q_raw, cos_t, sin_t).astype(jnp.bfloat16).astype(jnp.float32)
        keys = (rotate_half(k_raw, cos_t, sin_t) * KEY_DIM ** -0.5).astype(jnp.bfloat16).astype(jnp.float32)
        values = jnp.dot(h_one, w_v, preferred_element_type=jnp.float32).astype(jnp.bfloat16).astype(jnp.float32).reshape(CHUNK_LEN, NUM_HEADS, VAL_DIM)
        gates = jnp.dot(h_one, w_g, preferred_element_type=jnp.float32).reshape(CHUNK_LEN, NUM_HEADS, VAL_DIM)
        scores = jnp.einsum('chk,jhk->hcj', queries, keys) * inner_decay
        retained = jnp.einsum('hcj,jhe->che', scores, values) + jnp.einsum('chk,hke->che', queries, old_state) * query_decay[:, :, None]
        row_mean = jnp.mean(retained, axis=-1, keepdims=True)
        centered = retained - row_mean
        variance = jnp.mean(centered * centered, axis=-1, keepdims=True)
        normed = centered * lax.rsqrt(variance + GROUP_EPS)
        mixed = (jax.nn.silu(gates) * normed).astype(jnp.bfloat16).reshape(CHUNK_LEN, 2 * D_MODEL)
        attn_out = jnp.dot(mixed, w_o, preferred_element_type=jnp.float32).astype(jnp.bfloat16)
        x_mid = (x_f32 + attn_out.astype(jnp.float32)).astype(jnp.bfloat16)
        h_two = layer_norm(x_mid.astype(jnp.float32), ln2_gain, ln2_bias).astype(jnp.bfloat16)
        activated = jax.nn.gelu(jnp.dot(h_two, w_up, preferred_element_type=jnp.float32), approximate=False).astype(jnp.bfloat16)
        ffn_out = jnp.dot(activated, w_down, preferred_element_type=jnp.float32).astype(jnp.bfloat16)
        x_out = (x_mid.astype(jnp.float32) + ffn_out.astype(jnp.float32)).astype(jnp.bfloat16)
        new_state = state_decay[:, None, None] * old_state + jnp.einsum('jhk,jhe->hke', keys * key_decay[:, :, None], values)
        return x_out, new_state

    x_out, state_out = lax.map(one_sequence, (x_in, start_pos, kv_state))
    return (x_out, state_out)
```

```python
import functools

import jax
import jax.numpy as jnp
from jax import lax
from jax.experimental import pallas as pl
from jax.experimental.pallas import tpu as pltpu
from jax.sharding import PartitionSpec as P


NORM_EPS = 1e-5
GROUP_EPS = 1e-6
ROPE_BASE = 10000.0
TILE = 256
BF16 = jnp.bfloat16
F32 = jnp.float32


def dot(a, b):
    return jnp.dot(a, b, preferred_element_type=F32)


def layer_norm(x_f32, norm_gain, norm_bias):
    row_mean = jnp.mean(x_f32, axis=-1, keepdims=True)
    centered = x_f32 - row_mean
    variance = jnp.mean(centered * centered, axis=-1, keepdims=True)
    return centered * lax.rsqrt(variance + NORM_EPS) * norm_gain + norm_bias


def rope_block(base_ref, step_ref):
    cos_a, sin_a = base_ref[0, 0, 0:1, :], base_ref[0, 0, 1:2, :]
    cos_b, sin_b = step_ref[0], step_ref[1]
    return cos_a * cos_b - sin_a * sin_b, sin_a * cos_b + cos_a * sin_b


def rotate(v, cos_t, sin_t):
    half = v.shape[-1] // 2
    a, b = v[:, :half], v[:, half:]
    return jnp.concatenate([a * cos_t - b * sin_t, b * cos_t + a * sin_t], axis=-1)


def widen(row_table, width):
    return jnp.concatenate([row_table] * (width // row_table.shape[-1]), axis=-1)


def head_block(h, w_ref, state_ref, inner_ref, rows_ref, cos_t, sin_t):
    key_dim, val_dim = state_ref.shape[1], state_ref.shape[2]
    q_raw = dot(h, w_ref[:, :key_dim])
    k_raw = dot(h, w_ref[:, key_dim:2 * key_dim])
    values = dot(h, w_ref[:, 2 * key_dim:2 * key_dim + val_dim]).astype(BF16)
    gates = dot(h, w_ref[:, 2 * key_dim + val_dim:])
    queries = rotate(q_raw, cos_t, sin_t).astype(BF16)
    keys = (rotate(k_raw, cos_t, sin_t) * key_dim ** -0.5).astype(BF16)
    scores = lax.dot_general(queries, keys, (((1,), (1,)), ((), ())), preferred_element_type=F32) * inner_ref[0]
    state = state_ref[0]
    carried = dot(queries, state.astype(BF16)) * widen(rows_ref[0, 0], val_dim)
    retained = dot(scores.astype(BF16), values) + carried
    faded = (keys.astype(F32) * widen(rows_ref[0, 1], key_dim)).astype(BF16)
    update = lax.dot_general(faded, values, (((0,), (0,)), ((), ())), preferred_element_type=F32)
    state_ref[0] = state * widen(rows_ref[0, 2, 0:1], val_dim) + update
    row_mean = jnp.mean(retained, axis=-1, keepdims=True)
    centered = retained - row_mean
    variance = jnp.mean(centered * centered, axis=-1, keepdims=True)
    normed = centered * lax.rsqrt(variance + GROUP_EPS)
    return (gates * lax.logistic(gates) * normed).astype(BF16)


def load_state(in_ref, out_ref):
    @pl.when(pl.program_id(1) == 0)
    def _():
        out_ref[...] = in_ref[...]


def heads_kernel(ids_ref, x_ref, gain_ref, bias_ref, base_ref, step_ref, wa_ref, s_ref, inner_ref, rows_ref, z_ref, state_ref):
    load_state(s_ref, state_ref)
    h = layer_norm(x_ref[0].astype(F32), gain_ref[...], bias_ref[...]).astype(BF16)
    cos_t, sin_t = rope_block(base_ref, step_ref)
    z_ref[0] = head_block(h, wa_ref, state_ref, inner_ref, rows_ref, cos_t, sin_t)


def tail_kernel(ids_ref, x_ref, gain_ref, bias_ref, base_ref, step_ref, wa_ref, s_ref, inner_ref, rows_ref,
                z0_ref, z1_ref, z2_ref, gain2_ref, bias2_ref, wb0, wb1, wb2, wb3, *outs):
    whole_ref, out_ref, state_ref = outs[-3:]
    load_state(s_ref, state_ref)
    h = layer_norm(x_ref[0].astype(F32), gain_ref[...], bias_ref[...]).astype(BF16)
    cos_t, sin_t = rope_block(base_ref, step_ref)
    val_dim, d_model = z0_ref.shape[2], x_ref.shape[2]
    blocks = (wb0, wb1, wb2, wb3)
    mixed = (z0_ref[0], z1_ref[0], z2_ref[0], head_block(h, wa_ref, state_ref, inner_ref, rows_ref, cos_t, sin_t))
    u = sum(dot(z, wb[:val_dim, :d_model]) for z, wb in zip(mixed, blocks))
    x_mid = (x_ref[0].astype(F32) + u.astype(BF16).astype(F32)).astype(BF16)
    h_two = layer_norm(x_mid.astype(F32), gain2_ref[...], bias2_ref[...]).astype(BF16)
    f = jnp.zeros(u.shape, F32)
    for wb in blocks:
        up = dot(h_two, wb[:, d_model:])
        act = (up * 0.5 * (1.0 + lax.erf(up * 0.5 ** 0.5))).astype(BF16)
        f = f + dot(act, wb[val_dim:, :d_model])
    x_out = (x_mid.astype(F32) + f.astype(BF16).astype(F32)).astype(BF16)
    out_ref[0] = x_out
    whole_ref[0] = x_out


def resident(arr):
    return pl.BlockSpec(arr.shape, lambda s, t, ids: (0,) * arr.ndim, pipeline_mode=pl.Buffered(1))


def token_flops(d_model, key_dim, val_dim):
    return 2 * (d_model * (2 * key_dim + 2 * val_dim) + TILE * (key_dim + val_dim) + 2 * key_dim * val_dim)


def head_specs(x, gain, bias, rope_base, rope_step, wa, state, inner, rows):
    state_spec = pl.BlockSpec((1,) + state.shape[1:], lambda s, t, ids: (s, 0, 0))
    specs = [
        pl.BlockSpec((1, TILE, x.shape[2]), lambda s, t, ids: (ids[s], t, 0)),
        resident(gain), resident(bias),
        pl.BlockSpec((1, 1) + rope_base.shape[2:], lambda s, t, ids: (ids[s], t, 0, 0)),
        resident(rope_step), resident(wa), state_spec, resident(inner), resident(rows),
    ]
    return specs, [x, gain, bias, rope_base, rope_step, wa, state, inner, rows], state_spec


def call(body, ids, specs, args, outs, flops, byte_count, aliases):
    n, steps = ids.shape[0], args[0].shape[1] // TILE
    return pl.pallas_call(
        body,
        grid_spec=pltpu.PrefetchScalarGridSpec(num_scalar_prefetch=1, grid=(n, steps), in_specs=specs, out_specs=[spec for spec, _ in outs]),
        out_shape=[shape for _, shape in outs],
        compiler_params=pltpu.CompilerParams(dimension_semantics=("arbitrary", "arbitrary"), vmem_limit_bytes=58 << 20),
        cost_estimate=pl.CostEstimate(flops=n * steps * TILE * flops, bytes_accessed=n * steps * TILE * byte_count, transcendentals=0),
        input_output_aliases=aliases,
    )(ids, *args)


def tile_of(width, offset=0):
    return pl.BlockSpec((1, TILE, width), lambda s, t, ids: (s + offset, t, 0))


def run_heads(ids, *head_args):
    specs, args, state_spec = head_specs(*head_args)
    x, state = head_args[0], head_args[6]
    n, (key_dim, val_dim) = ids.shape[0], state.shape[1:]
    outs = [(tile_of(val_dim), jax.ShapeDtypeStruct((n, x.shape[1], val_dim), BF16)), (state_spec, jax.ShapeDtypeStruct((n, key_dim, val_dim), F32))]
    return call(heads_kernel, ids, specs, args, outs, token_flops(x.shape[2], key_dim, val_dim), 2 * (x.shape[2] + val_dim), {})


def run_tail(ids, whole, offsets, zs, gain2, bias2, wb, *head_args):
    specs, args, state_spec = head_specs(*head_args)
    x, state = head_args[0], head_args[6]
    n, (key_dim, val_dim), d_model = ids.shape[0], state.shape[1:], x.shape[2]
    specs += [tile_of(val_dim, offset) for offset in offsets]
    specs += [resident(arr) for arr in (gain2, bias2, *wb)]
    args += [*zs, gain2, bias2, *wb]
    aliases = {}
    if whole is not None:
        specs.append(pl.BlockSpec(memory_space=pl.ANY))
        args.append(whole)
        aliases = {len(args): 0}
    outs = [(pl.BlockSpec((1, TILE, d_model), lambda s, t, ids: (ids[s], t, 0)), jax.ShapeDtypeStruct(x.shape, BF16)),
            (tile_of(d_model), jax.ShapeDtypeStruct((n, x.shape[1], d_model), BF16)), (state_spec, jax.ShapeDtypeStruct((n, key_dim, val_dim), F32))]
    flops = token_flops(d_model, key_dim, val_dim) + 24 * d_model * val_dim
    return call(tail_kernel, ids, specs, args, outs, flops, 2 * (3 * d_model + 3 * val_dim), aliases)


def rope_tables(start_pos, chunk_len, key_dim):
    half_dim = key_dim // 2
    inv_freq = jnp.power(ROPE_BASE, -jnp.arange(half_dim).astype(F32) / half_dim)
    starts = (start_pos[:, None] + jnp.arange(0, chunk_len, TILE)[None, :]).astype(F32)
    base = starts[:, :, None] * inv_freq
    step = jnp.arange(TILE).astype(F32)[:, None] * inv_freq[None, :]
    return jnp.stack([jnp.cos(base), jnp.sin(base)], axis=2), jnp.stack([jnp.cos(step), jnp.sin(step)])


def decay_tables(head_ids):
    log_gamma = jnp.log1p(-jnp.exp2(-5.0 - head_ids.astype(F32)))[:, None, None]
    step_ids = jnp.arange(TILE)
    gap = step_ids[:, None] - step_ids[None, :]
    inner = jnp.where(gap[None] >= 0, jnp.exp(jnp.maximum(gap, 0).astype(F32)[None] * log_gamma), 0.0)
    lanes = jnp.zeros((1, 1, 128), F32)
    into = jnp.exp((step_ids + 1).astype(F32)[None, :, None] * log_gamma) + lanes
    out_of = jnp.exp((TILE - 1 - step_ids).astype(F32)[None, :, None] * log_gamma) + lanes
    over = jnp.exp(TILE * log_gamma) + jnp.zeros((1, TILE, 128), F32)
    return inner, jnp.stack([into, out_of, over], axis=1)


def solution(mesh):
    n_tp, n_dp = mesh.shape["tp"], mesh.shape["dp"]
    core_pairs = [(i, i ^ 1) for i in range(n_tp)]
    chip_pairs = [(i, i ^ 2) for i in range(n_tp)]
    far_pairs = [(i, i ^ 3) for i in range(n_tp)]

    def local_layer(x_in, start_pos, kv_state, ln1_gain, ln1_bias, w_q, w_k, w_v, w_g, w_o, ln2_gain, ln2_bias, w_up, w_down):
        to_core = functools.partial(lax.ppermute, axis_name="tp", perm=core_pairs)
        to_chip = functools.partial(lax.ppermute, axis_name="tp", perm=chip_pairs)
        to_far = functools.partial(lax.ppermute, axis_name="tp", perm=far_pairs)
        tp = lax.axis_index("tp")
        group = lax.axis_index("dp")
        chip, core = tp // 2, tp % 2
        other = 1 - core
        chunk_len = x_in.shape[1]
        states = kv_state[:, 0]
        key_dim, _ = states.shape[1:]

        def head_weights(part):
            return jnp.concatenate([part(w_q), part(w_k), part(w_v), part(w_g)], axis=1)

        def mlp_weights(part):
            pieces = [part(w_o), part(w_down), part(w_up)]
            return jnp.concatenate([jnp.concatenate(pieces[:2], axis=0), pieces[2]], axis=1)

        def quarter(w):
            rows = w.shape[0] // n_dp
            return lax.dynamic_slice_in_dim(w, group * rows, rows, axis=0)

        def gather(part):
            return lax.all_gather(part, "dp", axis=0, tiled=True)

        def pick(arr, i, n=1):
            return lax.dynamic_slice_in_dim(arr, i, n, axis=0)

        single, twice = 2 * chip + core, 4 + 2 * core
        single_o, twice_o = 2 * chip + other, 4 + 2 * other
        ids = jnp.stack([single, twice, twice + 1]).astype(jnp.int32)

        w_heads, w_mlp = head_weights(lambda w: w), mlp_weights(lambda w: w)
        wa_part = to_chip(head_weights(quarter))
        su_pair = to_chip(pick(states, 2 * (1 - chip), 2))
        wb_part = to_chip(quarter(w_mlp))
        st_pair = to_chip(states[4:8])
        wa_core = to_core(w_heads)
        s_core = to_core(jnp.concatenate([pick(states, single_o), pick(states, twice_o, 2)]))
        wb_core = to_core(w_mlp)

        row2 = lambda v: v.reshape(1, -1)
        rope_base, rope_step = rope_tables(start_pos, chunk_len, key_dim)
        inner, row_decay = decay_tables(jnp.stack([tp, tp ^ 1, tp ^ 2, tp ^ 3]))
        common = (x_in, row2(ln1_gain), row2(ln1_bias), rope_base, rope_step)

        def tables(i):
            return inner[i:i + 1], row_decay[i:i + 1]

        s_own = jnp.concatenate([pick(states, single), pick(states, twice, 2)])
        z_own, new_own = run_heads(ids, *common, w_heads, s_own, *tables(0))
        z_own, wa_core, s_core, wa_part, wb_part = lax.optimization_barrier((z_own, wa_core, s_core, wa_part, wb_part))
        wa_chip, wb_chip = gather(wa_part), gather(wb_part)
        z_core, new_core = run_heads(ids, *common, wa_core, s_core, *tables(1))
        got_core = to_core(new_core)

        z_core, wa_chip, wb_chip, su_pair, st_pair = lax.optimization_barrier((z_core, wa_chip, wb_chip, su_pair, st_pair))
        wa_far, wb_far = to_core(wa_chip), to_core(wb_chip)
        s_far = to_core(jnp.concatenate([pick(su_pair, other), pick(st_pair, 2 * other, 2)]))
        z_chip, new_chip = run_heads(ids[:1], *common, wa_chip, pick(su_pair, core), *tables(2))
        z_chip, wa_far, wb_far, wb_core, s_far = lax.optimization_barrier((z_chip, wa_far, wb_far, wb_core, s_far))

        mlp_args = (row2(ln2_gain), row2(ln2_bias), (w_mlp, wb_core, wb_chip, wb_far), *common, wa_far)
        whole, x_single, new_far = run_tail(ids[:1], None, (0, 0, 0), (z_own, z_core, z_chip), *mlp_args, s_far[:1], *tables(3))
        x_single_chip = to_chip(x_single)
        x_single_core = to_core(x_single)
        got_chip = to_chip(new_chip)
        got_far = to_far(new_far)
        whole, st_own, z_own = lax.optimization_barrier((whole, pick(st_pair, 2 * core, 2), z_own))
        z_chip, _ = run_heads(ids[1:], *common, wa_chip, st_own, *tables(2))
        whole, x_a, _ = run_tail(ids[1:2], whole, (1, 1, 0), (z_own, z_core, z_chip), *mlp_args, s_far[1:2], *tables(3))
        x_a_core = to_core(x_a)
        whole, x_b, _ = run_tail(ids[2:], whole, (2, 2, 1), (z_own, z_core, z_chip), *mlp_args, s_far[2:], *tables(3))
        x_b_core = to_core(x_b)
        x_single_far = to_core(x_single_chip)

        for block, i in ((x_single_core, single_o), (x_single_chip, 2 * (1 - chip) + core), (x_a_core, twice_o), (x_single_far, 2 * (1 - chip) + other), (x_b_core, twice_o + 1)):
            whole = lax.dynamic_update_slice_in_dim(whole, block, i, axis=0)

        def by_core(mine, theirs):
            return jnp.where(core == 0, jnp.concatenate([mine, theirs]), jnp.concatenate([theirs, mine]))

        mine = new_own
        near_pair, far_pair = by_core(mine[:1], got_core[:1]), by_core(got_chip, got_far)
        singles = jnp.where(chip == 0, jnp.concatenate([near_pair, far_pair]), jnp.concatenate([far_pair, near_pair]))
        new_states = jnp.concatenate([singles, by_core(mine[1:], got_core[1:])])
        return whole, new_states[:, None]

    in_specs = (P("dp", None, None), P("dp"), P("dp", "tp", None, None), P(), P(), P(None, "tp"), P(None, "tp"), P(None, "tp"), P(None, "tp"), P("tp", None), P(), P(), P(None, "tp"), P("tp", None))
    out_specs = (P("dp", None, None), P("dp", "tp", None, None))
    return jax.shard_map(local_layer, mesh=mesh, in_specs=in_specs, out_specs=out_specs, check_vma=False)
```

```python
import functools

import jax
import jax.numpy as jnp
from jax import lax
from jax.experimental import pallas as pl
from jax.experimental.pallas import tpu as pltpu
from jax.sharding import PartitionSpec as P


NORM_EPS = 1e-5
GROUP_EPS = 1e-6
ROPE_BASE = 10000.0
TILE = 256
BF16 = jnp.bfloat16
F32 = jnp.float32
ANY = pl.BlockSpec(memory_space=pl.ANY)


def dot(a, b):
    return jnp.dot(a, b, preferred_element_type=F32)


def layer_norm(x_f32, norm_gain, norm_bias):
    row_mean = jnp.mean(x_f32, axis=-1, keepdims=True)
    centered = x_f32 - row_mean
    variance = jnp.mean(centered * centered, axis=-1, keepdims=True)
    return centered * lax.rsqrt(variance + NORM_EPS) * norm_gain + norm_bias


def rotate(v, cos_t, sin_t):
    half = v.shape[-1] // 2
    a, b = v[:, :half], v[:, half:]
    return jnp.concatenate([a * cos_t - b * sin_t, b * cos_t + a * sin_t], axis=-1)


def widen(row_table, width):
    return jnp.concatenate([row_table] * (width // row_table.shape[-1]), axis=-1)


def decay_row(consts_ref, head):
    return consts_ref[5:6, 128 * head:128 * (head + 1)]


def fill_decays(consts_ref, heads, inner_ref, rows_ref):
    gap = lax.broadcasted_iota(jnp.int32, (TILE, TILE), 0) - lax.broadcasted_iota(jnp.int32, (TILE, TILE), 1)
    row = lax.broadcasted_iota(jnp.int32, (TILE, 128), 0)
    for i, head in enumerate(heads):
        log_gamma = decay_row(consts_ref, head)
        inner_ref[i] = jnp.where(gap >= 0, jnp.exp(jnp.maximum(gap, 0).astype(F32) * widen(log_gamma, TILE)), 0.0)
        rows_ref[i, 0] = jnp.exp((row + 1).astype(F32) * log_gamma)
        rows_ref[i, 1] = jnp.exp((TILE - 1 - row).astype(F32) * log_gamma)


def head_block(h, w_ref, s_ref, inner, rows_ref, over, cos_t, sin_t):
    key_dim, val_dim = s_ref.shape
    q_raw = dot(h, w_ref[:, :key_dim])
    k_raw = dot(h, w_ref[:, key_dim:2 * key_dim])
    values = dot(h, w_ref[:, 2 * key_dim:2 * key_dim + val_dim]).astype(BF16)
    gates = dot(h, w_ref[:, 2 * key_dim + val_dim:])
    queries = rotate(q_raw, cos_t, sin_t).astype(BF16)
    keys = (rotate(k_raw, cos_t, sin_t) * key_dim ** -0.5).astype(BF16)
    scores = lax.dot_general(queries, keys, (((1,), (1,)), ((), ())), preferred_element_type=F32) * inner
    state = s_ref[...]
    carried = dot(queries, state.astype(BF16)) * widen(rows_ref[0], val_dim)
    retained = dot(scores.astype(BF16), values) + carried
    faded = (keys.astype(F32) * widen(rows_ref[1], key_dim)).astype(BF16)
    update = lax.dot_general(faded, values, (((0,), (0,)), ((), ())), preferred_element_type=F32)
    s_ref[...] = state * widen(over, val_dim) + update
    row_mean = jnp.mean(retained, axis=-1, keepdims=True)
    centered = retained - row_mean
    variance = jnp.mean(centered * centered, axis=-1, keepdims=True)
    normed = centered * lax.rsqrt(variance + GROUP_EPS)
    return (gates * lax.logistic(gates) * normed).astype(BF16)


def kernel_body(heads, n_z, pieces, meta_ref, x_ref, consts_ref, base_ref, step_ref, *refs):
    n_heads = len(heads)
    it = iter(refs)

    def take(n):
        return [next(it) for _ in range(n)]

    s_refs, z_refs = take(n_heads), take(n_z)
    sources = [take(len(p)) for p in pieces]
    if n_z:
        take(len(refs) - (n_heads + n_z + sum(map(len, pieces)) + 2 + n_heads + 3 + len(pieces)))
        whole_ref, out_ref = take(2)
    else:
        z_ref = take(1)[0]
    state_refs = take(n_heads)
    inner_ref, rows_ref, sem = take(3)
    weights = take(len(pieces))

    @pl.when((pl.program_id(0) == 0) & (pl.program_id(1) == 0))
    def _():
        copies = []
        for w_ref, refs_in, places in zip(weights, sources, pieces):
            for ref, (row, col, flip) in zip(refs_in, places):
                if flip is not None:
                    row = pl.multiple_of((meta_ref[2, 0] ^ flip) * ref.shape[0], 256)
                dst = w_ref.at[pl.ds(row, ref.shape[0]), pl.ds(col, ref.shape[1])]
                copies.append(pltpu.make_async_copy(ref, dst, sem.at[len(copies)]))
                copies[-1].start()
        fill_decays(consts_ref, heads, inner_ref, rows_ref)
        for copy in copies:
            copy.wait()

    @pl.when(pl.program_id(1) == 0)
    def _():
        for s_ref, state_ref in zip(s_refs, state_refs):
            state_ref[...] = s_ref[...]

    h = layer_norm(x_ref[0].astype(F32), consts_ref[0:1, :], consts_ref[1:2, :]).astype(BF16)
    at = pl.multiple_of(pl.program_id(1) * 8, 8)
    cos_a, sin_a = base_ref[0, pl.ds(at, 1), :], base_ref[0, pl.ds(at + 1, 1), :]
    cos_b, sin_b = step_ref[0], step_ref[1]
    cos_t, sin_t = cos_a * cos_b - sin_a * sin_b, sin_a * cos_b + cos_a * sin_b
    mixed = []
    for i, head in enumerate(heads):
        over = jnp.exp(TILE * decay_row(consts_ref, head))
        mixed.append(head_block(h, weights[i], state_refs[i].at[0], inner_ref[i], rows_ref.at[i], over, cos_t, sin_t))
    if not n_z:
        z_ref[0] = mixed[0]
        return
    mixed = [z[0] for z in z_refs] + mixed
    blocks = weights[n_heads:]
    val_dim, d_model = mixed[0].shape[1], x_ref.shape[2]
    u = sum(dot(z, wb[:val_dim, :d_model]) for z, wb in zip(mixed, blocks))
    x_mid = (x_ref[0].astype(F32) + u.astype(BF16).astype(F32)).astype(BF16)
    h_two = layer_norm(x_mid.astype(F32), consts_ref[2:3, :], consts_ref[3:4, :]).astype(BF16)
    f = jnp.zeros(u.shape, F32)
    for wb in blocks:
        up = dot(h_two, wb[:, d_model:])
        act = (up * 0.5 * (1.0 + lax.erf(up * 0.5 ** 0.5))).astype(BF16)
        f = f + dot(act, wb[val_dim:, :d_model])
    x_out = (x_mid.astype(F32) + f.astype(BF16).astype(F32)).astype(BF16)
    out_ref[0] = x_out
    whole_ref[0] = x_out


def run(meta, common, heads, states, weights, zs=(), whole=None, states_whole=False):
    x, consts, base, step = common
    n, chunk_len, d_model = meta.shape[1], x.shape[1], x.shape[2]
    key_dim, val_dim = states[0].shape[1:]
    whole_spec = pl.BlockSpec((1, TILE, d_model), lambda s, t, m: (m[0, s], t, 0))
    state_in = pl.BlockSpec((1, key_dim, val_dim), lambda s, t, m: (m[1, s], 0, 0))
    state_out = pl.BlockSpec((1, key_dim, val_dim), lambda s, t, m: (m[0, s] if states_whole else s, 0, 0))

    def tile_of(width, offset=0):
        return pl.BlockSpec((1, TILE, width), lambda s, t, m: (s + offset, t, 0))

    def resident(arr):
        return pl.BlockSpec(arr.shape, lambda s, t, m: (0,) * arr.ndim, pipeline_mode=pl.Buffered(1))

    specs = [whole_spec, resident(consts), pl.BlockSpec((1,) + base.shape[1:], lambda s, t, m: (m[0, s], 0, 0)), resident(step)]
    specs += [state_in] * len(heads) + [tile_of(val_dim, offset) for _, offset in zs]
    args = [x, consts, base, step, *states, *(z for z, _ in zs)]
    pieces = []
    for weight in weights:
        pieces.append(tuple(place for _, place in weight))
        args += [arr for arr, _ in weight]
        specs += [ANY] * len(weight)
    aliases = {}
    if whole is not None:
        aliases = {len(args) + 1: 0}
        args.append(whole)
        specs.append(ANY)
    state_shape = jax.ShapeDtypeStruct((x.shape[0] if states_whole else n, key_dim, val_dim), F32)
    if zs:
        outs = [(whole_spec, jax.ShapeDtypeStruct(x.shape, BF16)), (tile_of(d_model), jax.ShapeDtypeStruct((n, chunk_len, d_model), BF16))]
    else:
        outs = [(tile_of(val_dim), jax.ShapeDtypeStruct((n, chunk_len, val_dim), BF16))]
    outs += [(state_out, state_shape)] * len(heads)
    flops = len(heads) * 2 * (d_model * (2 * key_dim + 2 * val_dim) + TILE * (key_dim + val_dim) + 2 * key_dim * val_dim)
    flops += 24 * d_model * val_dim if zs else 0
    n_copies = sum(map(len, pieces))
    return pl.pallas_call(
        functools.partial(kernel_body, tuple(heads), len(zs), tuple(pieces)),
        grid_spec=pltpu.PrefetchScalarGridSpec(
            num_scalar_prefetch=1, grid=(n, chunk_len // TILE), in_specs=specs, out_specs=[spec for spec, _ in outs],
            scratch_shapes=[pltpu.VMEM((len(heads), TILE, TILE), F32), pltpu.VMEM((len(heads), 2, TILE, 128), F32), pltpu.SemaphoreType.DMA((n_copies,))]
            + [pltpu.VMEM((d_model, 2 * key_dim + 2 * val_dim), BF16) for _ in weights]),
        out_shape=[shape for _, shape in outs],
        compiler_params=pltpu.CompilerParams(dimension_semantics=("arbitrary", "arbitrary"), vmem_limit_bytes=58 << 20),
        cost_estimate=pl.CostEstimate(flops=n * chunk_len * flops, bytes_accessed=n * chunk_len * d_model * (8 if zs else 4), transcendentals=0),
        input_output_aliases=aliases,
        name="tail" if zs else "heads",
    )(meta, *args)


def place_kernel(n_x, n_s, ids_ref, *refs):
    x_refs, s_refs = refs[:n_x], refs[n_x:n_x + n_s]
    whole_ref, states_ref, sem = refs[n_x + n_s + 2:]
    t = pl.program_id(0)
    copies = []
    for i, ref in enumerate(x_refs):
        copies.append(pltpu.make_async_copy(ref.at[0], whole_ref.at[ids_ref[i], pl.ds(pl.multiple_of(t * TILE, TILE), TILE), :], sem.at[i]))
    rows = s_refs[0].shape[1]
    for i, ref in enumerate(s_refs):
        copies.append(pltpu.make_async_copy(ref.at[0], states_ref.at[ids_ref[n_x + i], pl.ds(pl.multiple_of(t * rows, rows), rows), :], sem.at[n_x + i]))
    for copy in copies:
        copy.start()
    for copy in copies:
        copy.wait()


def place(ids, blocks, states, whole, new_states):
    steps = whole.shape[1] // TILE
    rows = new_states.shape[1] // steps

    def spec(height, width, at):
        return pl.BlockSpec((1, height, width), lambda t, m: (at, t, 0))

    specs = [spec(TILE, whole.shape[2], at) for _, at in blocks] + [spec(rows, new_states.shape[2], at) for _, at in states]
    n = len(specs)
    return pl.pallas_call(
        functools.partial(place_kernel, len(blocks), len(states)),
        grid_spec=pltpu.PrefetchScalarGridSpec(num_scalar_prefetch=1, grid=(steps,), in_specs=specs + [ANY, ANY], out_specs=[ANY, ANY],
                                               scratch_shapes=[pltpu.SemaphoreType.DMA((n,))]),
        out_shape=[jax.ShapeDtypeStruct(whole.shape, whole.dtype), jax.ShapeDtypeStruct(new_states.shape, new_states.dtype)],
        compiler_params=pltpu.CompilerParams(dimension_semantics=("arbitrary",), vmem_limit_bytes=32 << 20),
        input_output_aliases={n + 1: 0, n + 2: 1},
        name="place",
    )(ids, *(arr for arr, _ in blocks), *(arr for arr, _ in states), whole, new_states)


def rope_tables(start_pos, chunk_len, key_dim):
    half_dim = key_dim // 2
    inv_freq = jnp.power(ROPE_BASE, -jnp.arange(half_dim).astype(F32) / half_dim)
    starts = (start_pos[:, None] + jnp.arange(0, chunk_len, TILE)[None, :]).astype(F32)
    base = starts[:, :, None, None] * inv_freq
    row = lax.broadcasted_iota(jnp.int32, (1, 1, 8, 1), 2)
    base = jnp.where(row == 0, jnp.cos(base), jnp.sin(base))
    step = jnp.arange(TILE).astype(F32)[None, :, None] * inv_freq
    kind = lax.broadcasted_iota(jnp.int32, (2, 1, 1), 0)
    return base.reshape(start_pos.shape[0], -1, half_dim), jnp.where(kind == 0, jnp.cos(step), jnp.sin(step))


def solution(mesh):
    n_dp = mesh.shape["dp"]

    def swap(axis, bits):
        return functools.partial(lax.ppermute, axis_name=axis, perm=[(i, i ^ bits) for i in range(mesh.shape[axis])])

    to_core, to_chip, to_far = swap("tp", 1), swap("tp", 2), swap("tp", 3)

    def local_layer(x_in, start_pos, kv_state, ln1_gain, ln1_bias, w_q, w_k, w_v, w_g, w_o, ln2_gain, ln2_bias, w_up, w_down):
        tp, group = lax.axis_index("tp"), lax.axis_index("dp")
        chip, core = tp // 2, tp % 2
        other = 1 - core
        chunk_len, d_model = x_in.shape[1:]
        own = kv_state[:, 0]
        key_dim, val_dim = own.shape[1:]

        def rows_of(w, i, n):
            return lax.dynamic_slice_in_dim(w, i * n, n, axis=0)

        def quarter(w):
            return rows_of(w, group, w.shape[0] // n_dp)

        def head_places(arrs):
            return [(w, (0, col, None)) for w, col in zip(arrs, (0, key_dim, 2 * key_dim, 2 * key_dim + val_dim))]

        def mlp_places(arrs):
            return [(w, at) for w, at in zip(arrs, ((0, 0, None), (val_dim, 0, None), (0, d_model, None)))]

        def heads_gathered(quarters):
            return [(w, (0, 0, flip)) for flip, w in enumerate(quarters)]

        def gather(part):
            return [part] + [swap("dp", flip)(part) for flip in range(1, n_dp)]

        head_w, mlp_w = (w_q, w_k, w_v, w_g), (w_o, w_down, w_up)
        wa_part = to_chip(jnp.concatenate([quarter(w) for w in head_w], axis=1))
        wa_core = [to_core(w) for w in head_w]
        s_core = to_core(own)
        n_rows = d_model // n_dp
        stacked = jnp.where(group < n_dp // 2, rows_of(w_o, group % 2, n_rows), rows_of(w_down, group % 2, n_rows))
        wb_part = to_chip(jnp.concatenate([stacked, quarter(w_up)], axis=1))
        su_chip = to_chip(rows_of(own, 1 - chip, 2))
        st_chip = to_chip(own[4:8])
        wb_core = [to_core(w) for w in mlp_w]

        single, twice = 2 * chip + core, 4 + 2 * core
        single_o, twice_o = 2 * chip + other, 4 + 2 * other
        far_c, far_o = 2 * (1 - chip) + core, 2 * (1 - chip) + other

        def meta(seqs, rows):
            return jnp.stack([jnp.stack(seqs), jnp.stack(rows), jnp.stack([group] * len(seqs))]).astype(jnp.int32)

        m_single, m_twice = meta([single], [single]), meta([twice, twice + 1], [twice, twice + 1])
        m_three = meta([single, twice, twice + 1], [single, twice, twice + 1])
        m_far_single = meta([single], [core])
        m_a, m_b = meta([twice], [2 * core]), meta([twice + 1], [2 * core + 1])

        base, step = rope_tables(start_pos, chunk_len, key_dim)
        log_gamma = jnp.log1p(-jnp.exp2(-5.0 - jnp.stack([tp, tp ^ 1, tp ^ 2, tp ^ 3]).astype(F32)))
        spread = jnp.repeat(log_gamma, 128, total_repeat_length=4 * 128)
        consts = jnp.stack([ln1_gain, ln1_bias, ln2_gain, ln2_bias, jnp.zeros_like(ln1_gain)] + [jnp.pad(spread, (0, d_model - 4 * 128))] * 3)
        common = (x_in, consts, base, step)

        z_own_single, new_own_single = run(m_single, common, (0,), (own,), (head_places(head_w),))
        z_own_single, wa_part = lax.optimization_barrier((z_own_single, wa_part))
        wa_quarters = gather(wa_part)
        z_own, new_states = run(m_twice, common, (0,), (own,), (head_places(head_w),), states_whole=True)
        z_own, wa_core, s_core, wb_part = lax.optimization_barrier((z_own, wa_core, s_core, wb_part))
        wb_quarters = gather(wb_part)
        z_core, new_core = run(m_three, common, (1,), (s_core,), (head_places(wa_core),))
        z_core, wa_quarters, wb_quarters, su_chip, st_chip = lax.optimization_barrier((z_core, wa_quarters, wb_quarters, su_chip, st_chip))
        wa_far, su_far = [to_core(w) for w in wa_quarters], to_core(su_chip)
        wb_far, st_far = [to_core(w) for w in wb_quarters], to_core(st_chip)
        got_core = to_core(new_core)

        w_chip, w_far = heads_gathered(wa_quarters), heads_gathered(wa_far)
        z_chip, new_chip = run(m_far_single, common, (2,), (su_chip,), (w_chip,))
        z_chip, wa_far, wb_far, wb_core, su_far, st_far = lax.optimization_barrier((z_chip, wa_far, wb_far, wb_core, su_far, st_far))
        w_far = heads_gathered(wa_far)
        mlp = (mlp_places(mlp_w), mlp_places(wb_core), heads_gathered(wb_quarters), heads_gathered(wb_far))
        whole, x_single, new_far = run(m_far_single, common, (3,), (su_far,), (w_far, *mlp), ((z_own_single, 0), (z_core, 0), (z_chip, 0)))
        x_single_chip = to_chip(x_single)
        x_single_core = to_core(x_single)
        got_chip = to_chip(new_chip)
        got_far = to_far(new_far)
        far_states = (st_chip, st_far)
        whole, x_a, _, _ = run(m_a, common, (2, 3), far_states, (w_chip, w_far, *mlp), ((z_own, 0), (z_core, 1)), whole)
        x_a_core = to_core(x_a)
        whole, x_b, _, _ = run(m_b, common, (2, 3), far_states, (w_chip, w_far, *mlp), ((z_own, 1), (z_core, 2)), whole)
        x_b_core = to_core(x_b)
        x_single_far = to_core(x_single_chip)

        ids = jnp.stack([single_o, twice_o, far_c, far_o, twice_o + 1, single, single_o, twice_o, twice_o + 1, far_c, far_o])
        blocks = [(x_single_core, 0), (x_a_core, 0), (x_single_chip, 0), (x_single_far, 0), (x_b_core, 0)]
        new = [(new_own_single, 0), (got_core, 0), (got_core, 1), (got_core, 2), (got_chip, 0), (got_far, 0)]
        whole, new_states = place(ids.astype(jnp.int32), blocks, new, whole, new_states)
        return whole, new_states[:, None]

    in_specs = (P("dp", None, None), P("dp"), P("dp", "tp", None, None), P(), P(), P(None, "tp"), P(None, "tp"), P(None, "tp"), P(None, "tp"), P("tp", None), P(), P(), P(None, "tp"), P("tp", None))
    out_specs = (P("dp", None, None), P("dp", "tp", None, None))
    return jax.shard_map(local_layer, mesh=mesh, in_specs=in_specs, out_specs=out_specs, check_vma=False)
```

```python
import functools

import jax
import jax.numpy as jnp
import numpy as np
from jax import lax
from jax.experimental import pallas as pl
from jax.experimental.pallas import tpu as pltpu
from jax.sharding import PartitionSpec as P


NORM_EPS = 1e-5
GROUP_EPS = 1e-6
ROPE_BASE = 10000.0
TILE = 256
NUM_HEADS = 4
LOG_GAMMA = [float(np.log1p(-np.exp2(-5.0 - n))) for n in range(NUM_HEADS)]
SEQ, STATE_SINGLE, STATE_TWICE, GROUP, HEAD, PAIR, OTHER_CHIP = 0, 3, 4, 6, 7, 8, 9
BF16 = jnp.bfloat16
F32 = jnp.float32
ANY = pl.BlockSpec(memory_space=pl.ANY)


def dot(a, b):
    return jnp.dot(a, b, preferred_element_type=F32)


def layer_norm(x_f32, norm_gain, norm_bias):
    row_mean = jnp.mean(x_f32, axis=-1, keepdims=True)
    centered = x_f32 - row_mean
    variance = jnp.mean(centered * centered, axis=-1, keepdims=True)
    return centered * lax.rsqrt(variance + NORM_EPS) * norm_gain + norm_bias


def rotate(v, cos_t, sin_t):
    half = v.shape[-1] // 2
    a, b = v[:, :half], v[:, half:]
    return jnp.concatenate([a * cos_t - b * sin_t, b * cos_t + a * sin_t], axis=-1)


def widen(row_table, width):
    return jnp.concatenate([row_table] * (width // row_table.shape[-1]), axis=-1)


def log_decay(head):
    value = jnp.float32(LOG_GAMMA[0])
    for n, log_gamma in enumerate(LOG_GAMMA[1:], 1):
        value = jnp.where(head == n, jnp.float32(log_gamma), value)
    return value


def fill_decays(log_gammas, inner_ref, rows_ref):
    gap = lax.broadcasted_iota(jnp.int32, (TILE, TILE), 0) - lax.broadcasted_iota(jnp.int32, (TILE, TILE), 1)
    row = lax.broadcasted_iota(jnp.int32, (TILE, 128), 0)
    for i, log_gamma in enumerate(log_gammas):
        inner_ref[i] = jnp.where(gap >= 0, jnp.exp(jnp.maximum(gap, 0).astype(F32) * log_gamma), 0.0)
        rows_ref[i, 0] = jnp.exp((row + 1).astype(F32) * log_gamma)
        rows_ref[i, 1] = jnp.exp((TILE - 1 - row).astype(F32) * log_gamma)
        rows_ref[i, 2] = jnp.exp(jnp.full((TILE, 128), TILE, F32) * log_gamma)


def head_block(h, w_ref, s_ref, inner, rows_ref, cos_t, sin_t):
    key_dim, val_dim = s_ref.shape
    q_raw = dot(h, w_ref[:, :key_dim])
    k_raw = dot(h, w_ref[:, key_dim:2 * key_dim])
    queries = rotate(q_raw, cos_t, sin_t).astype(BF16)
    keys = (rotate(k_raw, cos_t, sin_t) * key_dim ** -0.5).astype(BF16)
    values = dot(h, w_ref[:, 2 * key_dim:2 * key_dim + val_dim]).astype(BF16)
    scores = lax.dot_general(queries, keys, (((1,), (1,)), ((), ())), preferred_element_type=F32) * inner
    state = s_ref[...]
    carried = dot(queries, state.astype(BF16)) * widen(rows_ref[0], val_dim)
    retained = dot(scores.astype(BF16), values) + carried
    gates = dot(h, w_ref[:, 2 * key_dim + val_dim:])
    faded = (keys.astype(F32) * widen(rows_ref[1], key_dim)).astype(BF16)
    update = lax.dot_general(faded, values, (((0,), (0,)), ((), ())), preferred_element_type=F32)
    s_ref[...] = state * widen(rows_ref[2, 0:1], val_dim) + update
    row_mean = jnp.mean(retained, axis=-1, keepdims=True)
    centered = retained - row_mean
    variance = jnp.mean(centered * centered, axis=-1, keepdims=True)
    normed = centered * lax.rsqrt(variance + GROUP_EPS)
    return (gates * lax.logistic(gates) * normed).astype(BF16)


def kernel_body(n_seqs, heads, n_z, pieces, with_whole, meta_ref, gain1, bias1, gain2, bias2, step_ref, *refs):
    it = iter(refs)

    def take(n):
        return [next(it) for _ in range(n)]

    x_refs, base_refs, s_refs, z_refs = take(n_seqs), take(n_seqs), [take(n_seqs) for _ in heads], take(n_z)
    sources = [take(len(p)) for p in pieces]
    take(with_whole)
    outs = take(2 if n_z else 1)
    state_refs = take(len(heads))
    inner_ref, rows_ref, sem = take(3)
    weights = take(len(pieces))

    @pl.when(pl.program_id(0) == 0)
    def _():
        copies = []
        for w_ref, refs_in, places in zip(weights, sources, pieces):
            for ref, (row, col, flip) in zip(refs_in, places):
                if flip is not None:
                    row = pl.multiple_of((meta_ref[GROUP] ^ flip) * ref.shape[0], 256)
                dst = w_ref.at[pl.ds(row, ref.shape[0]), pl.ds(col, ref.shape[1])]
                copies.append(pltpu.make_async_copy(ref, dst, sem.at[len(copies)]))
                copies[-1].start()
        fill_decays([log_decay(meta_ref[HEAD] ^ head) for head in heads], inner_ref, rows_ref)
        for per_head, state_ref in zip(s_refs, state_refs):
            for b, s_ref in enumerate(per_head):
                state_ref[b] = s_ref[0]
        for copy in copies:
            copy.wait()

    at = pl.multiple_of(pl.program_id(0) * 8, 8)
    cos_b, sin_b = step_ref[0], step_ref[1]
    normed, tables = [], []
    for x_ref, base_ref in zip(x_refs, base_refs):
        normed.append(layer_norm(x_ref[0].astype(F32), gain1[...], bias1[...]).astype(BF16))
        cos_a, sin_a = base_ref[0, pl.ds(at, 1), :], base_ref[0, pl.ds(at + 1, 1), :]
        tables.append((cos_a * cos_b - sin_a * sin_b, sin_a * cos_b + cos_a * sin_b))
    mixed = []
    for i in range(len(heads)):
        for b in range(n_seqs):
            mixed.append(head_block(normed[b], weights[i], state_refs[i].at[b], inner_ref[i], rows_ref.at[i], *tables[b]))
    if not n_z:
        for b in range(n_seqs):
            outs[0][b] = mixed[b]
        return
    mixed = [z[0] for z in z_refs] + mixed
    blocks = weights[len(heads):]
    val_dim, d_model = mixed[0].shape[1], x_refs[0].shape[2]
    u = sum(dot(z, wb[:val_dim, :d_model]) for z, wb in zip(mixed, blocks))
    x_mid = (x_refs[0][0].astype(F32) + u.astype(BF16).astype(F32)).astype(BF16)
    h_two = layer_norm(x_mid.astype(F32), gain2[...], bias2[...]).astype(BF16)
    f = jnp.zeros(u.shape, F32)
    for wb in blocks:
        up = dot(h_two, wb[:, d_model:])
        act = (up * 0.5 * (1.0 + lax.erf(up * 0.5 ** 0.5))).astype(BF16)
        f = f + dot(act, wb[val_dim:, :d_model])
    x_out = (x_mid.astype(F32) + f.astype(BF16).astype(F32)).astype(BF16)
    outs[0][0] = x_out
    outs[1][0] = x_out


def run(meta, common, seqs, state_rows, heads, states, weights, zs=(), whole=None, pair=False):
    x, norms, base, step = common
    n, chunk_len, d_model = len(seqs), x.shape[1], x.shape[2]
    key_dim, val_dim = states[0].shape[1:]

    def row_spec(shape, at):
        return pl.BlockSpec((1,) + shape, lambda t, m: (m[at], 0, 0))

    def token_spec(at):
        return pl.BlockSpec((1, TILE, d_model), lambda t, m: (m[at], t, 0))

    def tile_of(width, count=1, at=0):
        return pl.BlockSpec((count, TILE, width), lambda t, m: (at, t, 0))

    def resident(arr):
        return pl.BlockSpec(arr.shape, lambda t, m: (0,) * arr.ndim, pipeline_mode=pl.Buffered(1))

    specs = [resident(arr) for arr in (*norms, step)] + [token_spec(at) for at in seqs] + [row_spec(base.shape[1:], at) for at in seqs]
    args = [*norms, step] + [x] * n + [base] * n
    for state in states:
        specs += [row_spec(state.shape[1:], at) for at in state_rows]
        args += [state] * n
    specs += [tile_of(val_dim, 1, at) for _, at in zs]
    args += [z for z, _ in zs]
    pieces = []
    for weight in weights:
        pieces.append(tuple(place for _, place in weight))
        args += [arr for arr, _ in weight]
        specs += [ANY] * len(weight)
    aliases = {}
    if whole is not None:
        aliases = {len(args) + 1: 0}
        args.append(whole)
        specs.append(ANY)
    if zs:
        outs = [(token_spec(seqs[0]), jax.ShapeDtypeStruct(x.shape, BF16)), (tile_of(d_model), jax.ShapeDtypeStruct((1, chunk_len, d_model), BF16))]
    else:
        outs = [(tile_of(val_dim, n), jax.ShapeDtypeStruct((n, chunk_len, val_dim), BF16))]
    state_out = pl.BlockSpec((n, key_dim, val_dim), lambda t, m: (m[PAIR] if pair else 0, 0, 0))
    outs += [(state_out, jax.ShapeDtypeStruct((x.shape[0] if pair else n, key_dim, val_dim), F32))] * len(heads)
    flops = n * len(heads) * 2 * (d_model * (2 * key_dim + 2 * val_dim) + TILE * (key_dim + val_dim) + 2 * key_dim * val_dim)
    flops += 24 * d_model * val_dim if zs else 0
    return pl.pallas_call(
        functools.partial(kernel_body, n, tuple(heads), len(zs), tuple(pieces), whole is not None),
        grid_spec=pltpu.PrefetchScalarGridSpec(
            num_scalar_prefetch=1, grid=(chunk_len // TILE,), in_specs=specs, out_specs=[spec for spec, _ in outs],
            scratch_shapes=[pltpu.VMEM((len(heads), TILE, TILE), F32), pltpu.VMEM((len(heads), 3, TILE, 128), F32), pltpu.SemaphoreType.DMA((sum(map(len, pieces)),))]
            + [pltpu.VMEM((d_model, 2 * key_dim + 2 * val_dim), BF16) for _ in weights]),
        out_shape=[shape for _, shape in outs],
        compiler_params=pltpu.CompilerParams(dimension_semantics=("arbitrary",), vmem_limit_bytes=58 << 20),
        cost_estimate=pl.CostEstimate(flops=chunk_len * flops, bytes_accessed=n * chunk_len * d_model * (8 if zs else 4), transcendentals=0),
        input_output_aliases=aliases,
        name="tail" if zs else "heads",
    )(meta, *args)


def parts_kernel(meta_ref, w_q, w_k, w_v, w_g, w_o, w_down, w_up, own, heads_ref, mlp_ref, states_ref, sem):
    rows, group = heads_ref.shape[0], meta_ref[GROUP]
    at = pl.ds(pl.multiple_of(group * rows, rows), rows)
    half = pl.ds(pl.multiple_of((group % 2) * rows, rows), rows)
    d_model = w_o.shape[1]
    copies, col = [], 0
    for w in (w_q, w_k, w_v, w_g):
        copies.append(pltpu.make_async_copy(w.at[at], heads_ref.at[:, pl.ds(col, w.shape[1])], sem.at[len(copies)]))
        col += w.shape[1]
    copies.append(pltpu.make_async_copy(w_up.at[at], mlp_ref.at[:, pl.ds(d_model, w_up.shape[1])], sem.at[len(copies)]))
    copies.append(pltpu.make_async_copy(own.at[pl.ds(meta_ref[OTHER_CHIP], 2)], states_ref.at[pl.ds(0, 2)], sem.at[len(copies)]))
    copies.append(pltpu.make_async_copy(own.at[pl.ds(4, 4)], states_ref.at[pl.ds(2, 4)], sem.at[len(copies)]))
    for copy in copies:
        copy.start()
    last = [pltpu.make_async_copy(w.at[half], mlp_ref.at[:, pl.ds(0, d_model)], sem.at[len(copies)]) for w in (w_o, w_down)]

    @pl.when(group < 2)
    def _():
        last[0].start()

    @pl.when(group >= 2)
    def _():
        last[1].start()

    for copy in copies + last[:1]:
        copy.wait()


def cut_parts(meta, head_w, mlp_w, own):
    n_rows = mlp_w[0].shape[0] // 2
    shapes = [((n_rows, sum(w.shape[1] for w in head_w)), BF16), ((n_rows, mlp_w[0].shape[1] + mlp_w[2].shape[1]), BF16), ((6,) + own.shape[1:], F32)]
    return pl.pallas_call(
        parts_kernel,
        grid_spec=pltpu.PrefetchScalarGridSpec(num_scalar_prefetch=1, grid=(), in_specs=[ANY] * 8, out_specs=[pl.BlockSpec(memory_space=pltpu.VMEM)] * 3,
                                               scratch_shapes=[pltpu.SemaphoreType.DMA((8,))]),
        out_shape=[jax.ShapeDtypeStruct(shape, dtype) for shape, dtype in shapes],
        name="parts",
    )(meta, *head_w, *mlp_w, own)


def place_kernel(sources, n_wholes, ids_ref, *refs):
    in_refs, out_refs = refs[:len(sources)], refs[len(sources) + n_wholes:len(sources) + 2 * n_wholes]
    bufs, sem_in, sem_out = refs[len(sources) + 2 * n_wholes:-2], refs[-2], refs[-1]
    pulls, pushes, k = [], [], 0
    for i, ((seq, target, cuts), ref, buf) in enumerate(zip(sources, in_refs, bufs)):
        rows = buf.shape[0] // cuts
        for c in range(cuts):
            part = pl.ds(c * rows, rows)
            pulls.append(pltpu.make_async_copy(ref.at[seq, part], buf.at[part], sem_in.at[k]))
            pushes.append(pltpu.make_async_copy(buf.at[part], out_refs[target].at[ids_ref[i], part], sem_out.at[k]))
            k += 1
    for pull in pulls:
        pull.start()
    for pull, push in zip(pulls, pushes):
        pull.wait()
        push.start()
    for push in pushes:
        push.wait()


def place(ids, blocks, wholes):
    n, n_copies = len(blocks), sum(cuts for *_, cuts in blocks)
    return pl.pallas_call(
        functools.partial(place_kernel, tuple(block[1:] for block in blocks), len(wholes)),
        grid_spec=pltpu.PrefetchScalarGridSpec(
            num_scalar_prefetch=1, grid=(), in_specs=[ANY] * (n + len(wholes)), out_specs=[ANY] * len(wholes),
            scratch_shapes=[pltpu.VMEM(arr.shape[1:], arr.dtype) for arr, *_ in blocks] + [pltpu.SemaphoreType.DMA((n_copies,))] * 2),
        out_shape=[jax.ShapeDtypeStruct(arr.shape, arr.dtype) for arr in wholes],
        compiler_params=pltpu.CompilerParams(vmem_limit_bytes=40 << 20),
        input_output_aliases={1 + n + i: i for i in range(len(wholes))},
        name="place",
    )(ids, *(arr for arr, *_ in blocks), *wholes)


def rope_tables(start_pos, chunk_len, key_dim):
    half_dim = key_dim // 2
    inv_freq = jnp.power(ROPE_BASE, -jnp.arange(half_dim).astype(F32) / half_dim)
    starts = (start_pos[:, None] + jnp.arange(0, chunk_len, TILE)[None, :]).astype(F32)
    base = starts[:, :, None, None] * inv_freq
    row = lax.broadcasted_iota(jnp.int32, (1, 1, 8, 1), 2)
    base = jnp.where(row == 0, jnp.cos(base), jnp.sin(base))
    step = jnp.arange(TILE).astype(F32)[None, :, None] * inv_freq
    kind = lax.broadcasted_iota(jnp.int32, (2, 1, 1), 0)
    return base.reshape(start_pos.shape[0], -1, half_dim), jnp.where(kind == 0, jnp.cos(step), jnp.sin(step))


def solution(mesh):
    n_dp = mesh.shape["dp"]

    def swap(axis, bits):
        return functools.partial(lax.ppermute, axis_name=axis, perm=[(i, i ^ bits) for i in range(mesh.shape[axis])])

    to_core, to_chip, to_far = swap("tp", 1), swap("tp", 2), swap("tp", 3)

    def local_layer(x_in, start_pos, kv_state, ln1_gain, ln1_bias, w_q, w_k, w_v, w_g, w_o, ln2_gain, ln2_bias, w_up, w_down):
        tp, group = lax.axis_index("tp"), lax.axis_index("dp")
        chip, core = tp // 2, tp % 2
        other = 1 - core
        chunk_len, d_model = x_in.shape[1:]
        own = kv_state[:, 0]
        key_dim, val_dim = own.shape[1:]

        def head_places(arrs):
            return [(w, (0, col, None)) for w, col in zip(arrs, (0, key_dim, 2 * key_dim, 2 * key_dim + val_dim))]

        def mlp_places(arrs):
            return [(w, at) for w, at in zip(arrs, ((0, 0, None), (val_dim, 0, None), (0, d_model, None)))]

        def heads_gathered(quarters):
            return [(w, (0, 0, flip)) for flip, w in enumerate(quarters)]

        def gather(part):
            return [part] + [swap("dp", flip)(part) for flip in range(1, n_dp)]

        head_w, mlp_w = (w_q, w_k, w_v, w_g), (w_o, w_down, w_up)
        single, twice = 2 * chip + core, 4 + 2 * core
        meta = jnp.stack([single, twice, twice + 1, core, 2 + 2 * core, 3 + 2 * core, group, tp, twice // 2, 2 * (1 - chip)]).astype(jnp.int32)
        wa_core = [to_core(w) for w in head_w]
        s_core = to_core(own)
        wa_part, wb_part, s_part = cut_parts(meta, head_w, mlp_w, own)
        wa_part = to_chip(wa_part)
        wb_part = to_chip(wb_part)
        s_chip = to_chip(s_part)
        wb_core = [to_core(w) for w in mlp_w]

        norms = tuple(v.reshape(1, -1) for v in (ln1_gain, ln1_bias, ln2_gain, ln2_bias))
        common = (x_in, norms, *rope_tables(start_pos, chunk_len, key_dim))
        all_seqs, pair_seqs, one = (SEQ, SEQ + 1, SEQ + 2), (SEQ + 1, SEQ + 2), (SEQ,)

        z_own_single, new_own_single = run(meta, common, one, one, (0,), (own,), (head_places(head_w),))
        z_own_single, wa_part = lax.optimization_barrier((z_own_single, wa_part))
        wa_quarters = gather(wa_part)
        z_own, new_states = run(meta, common, pair_seqs, pair_seqs, (0,), (own,), (head_places(head_w),), pair=True)
        z_own, wa_core, s_core, wb_part = lax.optimization_barrier((z_own, wa_core, s_core, wb_part))
        wb_quarters = gather(wb_part)
        z_core, new_core = run(meta, common, all_seqs, all_seqs, (1,), (s_core,), (head_places(wa_core),))
        z_core, wa_quarters, wb_quarters, s_chip = lax.optimization_barrier((z_core, wa_quarters, wb_quarters, s_chip))
        wa_far, wb_far, s_far = [to_core(w) for w in wa_quarters], [to_core(w) for w in wb_quarters], to_core(s_chip)
        got_core = to_core(new_core)

        w_chip = heads_gathered(wa_quarters)
        z_chip, new_chip = run(meta, common, one, (STATE_SINGLE,), (2,), (s_chip,), (w_chip,))
        z_chip, wa_far, wb_far, wb_core, s_far = lax.optimization_barrier((z_chip, wa_far, wb_far, wb_core, s_far))
        w_far = heads_gathered(wa_far)
        mlp = (mlp_places(mlp_w), mlp_places(wb_core), heads_gathered(wb_quarters), heads_gathered(wb_far))
        whole, x_single, new_far = run(meta, common, one, (STATE_SINGLE,), (3,), (s_far,), (w_far, *mlp), ((z_own_single, 0), (z_core, 0), (z_chip, 0)))
        x_single_chip = to_chip(x_single)
        x_single_core = to_core(x_single)
        got_chip = to_chip(new_chip)
        got_far = to_far(new_far)
        far = ((2, 3), (s_chip, s_far), (w_chip, w_far, *mlp))
        whole, x_a, _, _ = run(meta, common, (SEQ + 1,), (STATE_TWICE,), *far, ((z_own, 0), (z_core, 1)), whole)
        x_a_core = to_core(x_a)
        whole, x_b, _, _ = run(meta, common, (SEQ + 2,), (STATE_TWICE + 1,), *far, ((z_own, 1), (z_core, 2)), whole)
        x_b_core = to_core(x_b)
        x_single_far = to_core(x_single_chip)

        single_o, twice_o = 2 * chip + other, 4 + 2 * other
        far_c, far_o = 2 * (1 - chip) + core, 2 * (1 - chip) + other
        ids = jnp.stack([single_o, twice_o, far_c, single, single_o, twice_o, twice_o + 1, far_c, far_o, far_o, twice_o + 1]).astype(jnp.int32)
        cuts = chunk_len // TILE
        near = [(x_single_core, 0, 0, cuts), (x_a_core, 0, 0, cuts), (x_single_chip, 0, 0, cuts)]
        near += [(arr, at, 1, 1) for arr, at in ((new_own_single, 0), (got_core, 0), (got_core, 1), (got_core, 2), (got_chip, 0), (got_far, 0))]
        whole, new_states = place(ids[:9], near, (whole, new_states))
        whole, = place(ids[9:], [(x_single_far, 0, 0, cuts), (x_b_core, 0, 0, cuts)], (whole,))
        return whole, new_states[:, None]

    in_specs = (P("dp", None, None), P("dp"), P("dp", "tp", None, None), P(), P(), P(None, "tp"), P(None, "tp"), P(None, "tp"), P(None, "tp"), P("tp", None), P(), P(), P(None, "tp"), P("tp", None))
    out_specs = (P("dp", None, None), P("dp", "tp", None, None))
    return jax.shard_map(local_layer, mesh=mesh, in_specs=in_specs, out_specs=out_specs, check_vma=False)
```

```python
import functools

import jax
import jax.numpy as jnp
import numpy as np
from jax import lax
from jax.experimental import pallas as pl
from jax.experimental.pallas import tpu as pltpu
from jax.sharding import PartitionSpec as P


NORM_EPS = 1e-5
GROUP_EPS = 1e-6
ROPE_BASE = 10000.0
TILE = 256
NUM_HEADS = 4
LOG_GAMMA = [float(np.log1p(-np.exp2(-5.0 - n))) for n in range(NUM_HEADS)]
SEQ, STATE_SINGLE, STATE_TWICE, GROUP, HEAD, PAIR, OTHER_CHIP = 0, 3, 4, 6, 7, 8, 9
BF16 = jnp.bfloat16
F32 = jnp.float32
ANY = pl.BlockSpec(memory_space=pl.ANY)


def dot(a, b):
    return jnp.dot(a, b, preferred_element_type=F32)


def layer_norm(x_f32, norm_gain, norm_bias):
    row_mean = jnp.mean(x_f32, axis=-1, keepdims=True)
    centered = x_f32 - row_mean
    variance = jnp.mean(centered * centered, axis=-1, keepdims=True)
    return centered * lax.rsqrt(variance + NORM_EPS) * norm_gain + norm_bias


def rotate(v, cos_t, sin_t):
    half = v.shape[-1] // 2
    a, b = v[:, :half], v[:, half:]
    return jnp.concatenate([a * cos_t - b * sin_t, b * cos_t + a * sin_t], axis=-1)


def widen(row_table, width):
    return jnp.concatenate([row_table] * (width // row_table.shape[-1]), axis=-1)


def log_decay(head):
    value = jnp.float32(LOG_GAMMA[0])
    for n, log_gamma in enumerate(LOG_GAMMA[1:], 1):
        value = jnp.where(head == n, jnp.float32(log_gamma), value)
    return value


def fill_decays(log_gammas, inner_ref, rows_ref):
    gap = lax.broadcasted_iota(jnp.int32, (TILE, TILE), 0) - lax.broadcasted_iota(jnp.int32, (TILE, TILE), 1)
    row = lax.broadcasted_iota(jnp.int32, (TILE, 128), 0)
    for i, log_gamma in enumerate(log_gammas):
        inner_ref[i] = jnp.where(gap >= 0, jnp.exp(jnp.maximum(gap, 0).astype(F32) * log_gamma), 0.0)
        rows_ref[i, 0] = jnp.exp((row + 1).astype(F32) * log_gamma)
        rows_ref[i, 1] = jnp.exp((TILE - 1 - row).astype(F32) * log_gamma)
        rows_ref[i, 2] = jnp.exp(jnp.full((TILE, 128), TILE, F32) * log_gamma)


def head_blocks(hs, w_ref, state_ref, inner, rows_ref, tables):
    _, key_dim, val_dim = state_ref.shape
    out = []
    for b, h in enumerate(hs):
        q_raw = dot(h, w_ref[:, :key_dim])
        k_raw = dot(h, w_ref[:, key_dim:2 * key_dim])
        queries = rotate(q_raw, *tables[b]).astype(BF16)
        keys = (rotate(k_raw, *tables[b]) * key_dim ** -0.5).astype(BF16)
        values = dot(h, w_ref[:, 2 * key_dim:2 * key_dim + val_dim]).astype(BF16)
        scores = lax.dot_general(queries, keys, (((1,), (1,)), ((), ())), preferred_element_type=F32) * inner
        state = state_ref[b]
        carried = dot(queries, state.astype(BF16)) * widen(rows_ref[0], val_dim)
        retained = dot(scores.astype(BF16), values) + carried
        gates = dot(h, w_ref[:, 2 * key_dim + val_dim:])
        faded = (keys.astype(F32) * widen(rows_ref[1], key_dim)).astype(BF16)
        update = lax.dot_general(faded, values, (((0,), (0,)), ((), ())), preferred_element_type=F32)
        state_ref[b] = state * widen(rows_ref[2, 0:1], val_dim) + update
        row_mean = jnp.mean(retained, axis=-1, keepdims=True)
        centered = retained - row_mean
        variance = jnp.mean(centered * centered, axis=-1, keepdims=True)
        normed = centered * lax.rsqrt(variance + GROUP_EPS)
        out.append((gates * lax.logistic(gates) * normed).astype(BF16))
    return out


def kernel_body(n_seqs, heads, n_z, pieces, with_whole, meta_ref, gain1, bias1, gain2, bias2, step_ref, *refs):
    it = iter(refs)

    def take(n):
        return [next(it) for _ in range(n)]

    x_refs, base_refs, s_refs, z_refs = take(n_seqs), take(n_seqs), [take(n_seqs) for _ in heads], [take(n_seqs) for _ in range(n_z)]
    sources = [take(len(p)) for p in pieces]
    take(with_whole)
    outs = take(1 + n_seqs if n_z else 1)
    state_refs = take(len(heads))
    inner_ref, rows_ref, sem = take(3)
    weights = take(len(pieces))

    @pl.when(pl.program_id(0) == 0)
    def _():
        copies = []
        for w_ref, refs_in, places in zip(weights, sources, pieces):
            for ref, (row, col, flip) in zip(refs_in, places):
                if flip is not None:
                    row = pl.multiple_of((meta_ref[GROUP] ^ flip) * ref.shape[0], 256)
                dst = w_ref.at[pl.ds(row, ref.shape[0]), pl.ds(col, ref.shape[1])]
                copies.append(pltpu.make_async_copy(ref, dst, sem.at[len(copies)]))
                copies[-1].start()
        fill_decays([log_decay(meta_ref[HEAD] ^ head) for head in heads], inner_ref, rows_ref)
        for per_head, state_ref in zip(s_refs, state_refs):
            for b, s_ref in enumerate(per_head):
                state_ref[b] = s_ref[0]
        for copy in copies:
            copy.wait()

    at = pl.multiple_of(pl.program_id(0) * 8, 8)
    cos_b, sin_b = step_ref[0], step_ref[1]
    normed, tables = [], []
    for x_ref, base_ref in zip(x_refs, base_refs):
        normed.append(layer_norm(x_ref[0].astype(F32), gain1[...], bias1[...]).astype(BF16))
        cos_a, sin_a = base_ref[0, pl.ds(at, 1), :], base_ref[0, pl.ds(at + 1, 1), :]
        tables.append((cos_a * cos_b - sin_a * sin_b, sin_a * cos_b + cos_a * sin_b))
    mixed = [head_blocks(normed, weights[i], state_refs[i], inner_ref[i], rows_ref.at[i], tables) for i in range(len(heads))]
    if not n_z:
        for b in range(n_seqs):
            outs[0][b] = mixed[0][b]
        return
    mixed = [[ref[0] for ref in refs_of] for refs_of in z_refs] + mixed
    blocks = weights[len(heads):]
    val_dim, d_model = mixed[0][0].shape[1], x_refs[0].shape[2]
    u = sum(dot(below(z), wb[:val_dim, :d_model]) for z, wb in zip(mixed, blocks))
    x_mid = (below([x_ref[0] for x_ref in x_refs]).astype(F32) + u.astype(BF16).astype(F32)).astype(BF16)
    h_two = layer_norm(x_mid.astype(F32), gain2[...], bias2[...]).astype(BF16)
    f = jnp.zeros(u.shape, F32)
    for wb in blocks:
        up = dot(h_two, wb[:, d_model:])
        act = (up * 0.5 * (1.0 + lax.erf(up * 0.5 ** 0.5))).astype(BF16)
        f = f + dot(act, wb[val_dim:, :d_model])
    x_out = (x_mid.astype(F32) + f.astype(BF16).astype(F32)).astype(BF16)
    for b in range(n_seqs):
        outs[0][b] = x_out[b * TILE:(b + 1) * TILE]
        outs[1 + b][0] = x_out[b * TILE:(b + 1) * TILE]


def below(blocks):
    return blocks[0] if len(blocks) == 1 else jnp.concatenate(blocks, axis=0)


def run(meta, common, seqs, state_rows, heads, states, weights, zs=(), whole=None, pair=False):
    x, norms, base, step = common
    n, chunk_len, d_model = len(seqs), x.shape[1], x.shape[2]
    key_dim, val_dim = states[0].shape[1:]

    def row_spec(shape, at):
        return pl.BlockSpec((1,) + shape, lambda t, m: (m[at], 0, 0))

    def token_spec(at):
        return pl.BlockSpec((1, TILE, d_model), lambda t, m: (m[at], t, 0))

    def tile_of(width, count=1, at=0):
        return pl.BlockSpec((count, TILE, width), lambda t, m: (at, t, 0))

    def resident(arr):
        return pl.BlockSpec(arr.shape, lambda t, m: (0,) * arr.ndim, pipeline_mode=pl.Buffered(1))

    specs = [resident(arr) for arr in (*norms, step)] + [token_spec(at) for at in seqs] + [row_spec(base.shape[1:], at) for at in seqs]
    args = [*norms, step] + [x] * n + [base] * n
    for state in states:
        specs += [row_spec(state.shape[1:], at) for at in state_rows]
        args += [state] * n
    for z, first in zs:
        specs += [tile_of(val_dim, 1, first + b) for b in range(n)]
        args += [z] * n
    pieces = []
    for weight in weights:
        pieces.append(tuple(place for _, place in weight))
        args += [arr for arr, _ in weight]
        specs += [ANY] * len(weight)
    aliases = {}
    if whole is not None:
        aliases = {len(args) + 1: 0}
        args.append(whole)
        specs.append(ANY)
    if zs:
        whole_spec = token_spec(seqs[0]) if n == 1 else pl.BlockSpec((n, TILE, d_model), lambda t, m: (m[PAIR], t, 0))
        outs = [(whole_spec, jax.ShapeDtypeStruct(x.shape, BF16))] + [(tile_of(d_model), jax.ShapeDtypeStruct((1, chunk_len, d_model), BF16))] * n
    else:
        outs = [(tile_of(val_dim, n), jax.ShapeDtypeStruct((n, chunk_len, val_dim), BF16))]
    state_out = pl.BlockSpec((n, key_dim, val_dim), lambda t, m: (m[PAIR] if pair else 0, 0, 0))
    outs += [(state_out, jax.ShapeDtypeStruct((x.shape[0] if pair else n, key_dim, val_dim), F32))] * len(heads)
    flops = n * len(heads) * 2 * (d_model * (2 * key_dim + 2 * val_dim) + TILE * (key_dim + val_dim) + 2 * key_dim * val_dim)
    flops += n * 24 * d_model * val_dim if zs else 0
    return pl.pallas_call(
        functools.partial(kernel_body, n, tuple(heads), len(zs), tuple(pieces), whole is not None),
        grid_spec=pltpu.PrefetchScalarGridSpec(
            num_scalar_prefetch=1, grid=(chunk_len // TILE,), in_specs=specs, out_specs=[spec for spec, _ in outs],
            scratch_shapes=[pltpu.VMEM((len(heads), TILE, TILE), F32), pltpu.VMEM((len(heads), 3, TILE, 128), F32), pltpu.SemaphoreType.DMA((sum(map(len, pieces)),))]
            + [pltpu.VMEM((d_model, 2 * key_dim + 2 * val_dim), BF16) for _ in weights]),
        out_shape=[shape for _, shape in outs],
        compiler_params=pltpu.CompilerParams(dimension_semantics=("arbitrary",), vmem_limit_bytes=58 << 20),
        cost_estimate=pl.CostEstimate(flops=chunk_len * flops, bytes_accessed=n * chunk_len * d_model * (8 if zs else 4), transcendentals=0),
        input_output_aliases=aliases,
        name="tail" if zs else "heads",
    )(meta, *args)


def parts_kernel(meta_ref, w_q, w_k, w_v, w_g, w_o, w_down, w_up, own, heads_ref, mlp_ref, single_ref, twice_ref, sem):
    rows, group = heads_ref.shape[0], meta_ref[GROUP]
    at = pl.ds(pl.multiple_of(group * rows, rows), rows)
    half = pl.ds(pl.multiple_of((group % 2) * rows, rows), rows)
    d_model = w_o.shape[1]
    copies, col = [], 0
    for w in (w_q, w_k, w_v, w_g):
        copies.append(pltpu.make_async_copy(w.at[at], heads_ref.at[:, pl.ds(col, w.shape[1])], sem.at[len(copies)]))
        col += w.shape[1]
    copies.append(pltpu.make_async_copy(w_up.at[at], mlp_ref.at[:, pl.ds(d_model, w_up.shape[1])], sem.at[len(copies)]))
    copies.append(pltpu.make_async_copy(own.at[pl.ds(meta_ref[OTHER_CHIP], 2)], single_ref, sem.at[len(copies)]))
    copies.append(pltpu.make_async_copy(own.at[pl.ds(4, 4)], twice_ref, sem.at[len(copies)]))
    for copy in copies:
        copy.start()
    last = [pltpu.make_async_copy(w.at[half], mlp_ref.at[:, pl.ds(0, d_model)], sem.at[len(copies)]) for w in (w_o, w_down)]

    @pl.when(group < 2)
    def _():
        last[0].start()

    @pl.when(group >= 2)
    def _():
        last[1].start()

    for copy in copies + last[:1]:
        copy.wait()


def cut_parts(meta, head_w, mlp_w, own):
    n_rows = mlp_w[0].shape[0] // 2
    shapes = [((n_rows, sum(w.shape[1] for w in head_w)), BF16), ((n_rows, mlp_w[0].shape[1] + mlp_w[2].shape[1]), BF16), ((2,) + own.shape[1:], F32), ((4,) + own.shape[1:], F32)]
    return pl.pallas_call(
        parts_kernel,
        grid_spec=pltpu.PrefetchScalarGridSpec(num_scalar_prefetch=1, grid=(), in_specs=[ANY] * 8, out_specs=[pl.BlockSpec(memory_space=pltpu.VMEM)] * 4,
                                               scratch_shapes=[pltpu.SemaphoreType.DMA((8,))]),
        out_shape=[jax.ShapeDtypeStruct(shape, dtype) for shape, dtype in shapes],
        name="parts",
    )(meta, *head_w, *mlp_w, own)


def place_kernel(sources, n_wholes, ids_ref, *refs):
    in_refs, out_refs = refs[:len(sources)], refs[len(sources) + n_wholes:len(sources) + 2 * n_wholes]
    bufs, sem_in, sem_out = refs[len(sources) + 2 * n_wholes:-2], refs[-2], refs[-1]
    pulls, pushes, k = [], [], 0
    for i, ((seq, target, cuts), ref, buf) in enumerate(zip(sources, in_refs, bufs)):
        rows = buf.shape[0] // cuts
        for c in range(cuts):
            part = pl.ds(c * rows, rows)
            pulls.append(pltpu.make_async_copy(ref.at[seq, part], buf.at[part], sem_in.at[k]))
            pushes.append(pltpu.make_async_copy(buf.at[part], out_refs[target].at[ids_ref[i], part], sem_out.at[k]))
            k += 1
    for pull in pulls:
        pull.start()
    for pull, push in zip(pulls, pushes):
        pull.wait()
        push.start()
    for push in pushes:
        push.wait()


def place(ids, blocks, wholes):
    n, n_copies = len(blocks), sum(cuts for *_, cuts in blocks)
    return pl.pallas_call(
        functools.partial(place_kernel, tuple(block[1:] for block in blocks), len(wholes)),
        grid_spec=pltpu.PrefetchScalarGridSpec(
            num_scalar_prefetch=1, grid=(), in_specs=[ANY] * (n + len(wholes)), out_specs=[ANY] * len(wholes),
            scratch_shapes=[pltpu.VMEM(arr.shape[1:], arr.dtype) for arr, *_ in blocks] + [pltpu.SemaphoreType.DMA((n_copies,))] * 2),
        out_shape=[jax.ShapeDtypeStruct(arr.shape, arr.dtype) for arr in wholes],
        compiler_params=pltpu.CompilerParams(vmem_limit_bytes=40 << 20),
        input_output_aliases={1 + n + i: i for i in range(len(wholes))},
        name="place",
    )(ids, *(arr for arr, *_ in blocks), *wholes)


def rope_tables(start_pos, chunk_len, key_dim):
    half_dim = key_dim // 2
    inv_freq = jnp.power(ROPE_BASE, -jnp.arange(half_dim).astype(F32) / half_dim)
    starts = (start_pos[:, None] + jnp.arange(0, chunk_len, TILE)[None, :]).astype(F32)
    base = starts[:, :, None, None] * inv_freq
    row = lax.broadcasted_iota(jnp.int32, (1, 1, 8, 1), 2)
    base = jnp.where(row == 0, jnp.cos(base), jnp.sin(base))
    step = jnp.arange(TILE).astype(F32)[None, :, None] * inv_freq
    kind = lax.broadcasted_iota(jnp.int32, (2, 1, 1), 0)
    return base.reshape(start_pos.shape[0], -1, half_dim), jnp.where(kind == 0, jnp.cos(step), jnp.sin(step))


def solution(mesh):
    n_dp = mesh.shape["dp"]

    def swap(axis, bits):
        return functools.partial(lax.ppermute, axis_name=axis, perm=[(i, i ^ bits) for i in range(mesh.shape[axis])])

    to_core, to_chip, to_far = swap("tp", 1), swap("tp", 2), swap("tp", 3)

    def local_layer(x_in, start_pos, kv_state, ln1_gain, ln1_bias, w_q, w_k, w_v, w_g, w_o, ln2_gain, ln2_bias, w_up, w_down):
        tp, group = lax.axis_index("tp"), lax.axis_index("dp")
        chip, core = tp // 2, tp % 2
        other = 1 - core
        chunk_len, d_model = x_in.shape[1:]
        own = kv_state[:, 0]
        key_dim, val_dim = own.shape[1:]

        def head_places(arrs):
            return [(w, (0, col, None)) for w, col in zip(arrs, (0, key_dim, 2 * key_dim, 2 * key_dim + val_dim))]

        def mlp_places(arrs):
            return [(w, at) for w, at in zip(arrs, ((0, 0, None), (val_dim, 0, None), (0, d_model, None)))]

        def heads_gathered(quarters):
            return [(w, (0, 0, flip)) for flip, w in enumerate(quarters)]

        def gather(part):
            return [part] + [swap("dp", flip)(part) for flip in range(1, n_dp)]

        head_w, mlp_w = (w_q, w_k, w_v, w_g), (w_o, w_down, w_up)
        single, twice = 2 * chip + core, 4 + 2 * core
        meta = jnp.stack([single, twice, twice + 1, core, 2 * core, 2 * core + 1, group, tp, twice // 2, 2 * (1 - chip)]).astype(jnp.int32)
        wa_core = [to_core(w) for w in head_w]
        s_core = to_core(own)
        wa_part, wb_part, su_part, st_part = cut_parts(meta, head_w, mlp_w, own)
        wa_part = to_chip(wa_part)
        wb_part = to_chip(wb_part)
        su_chip = to_chip(su_part)
        st_chip = to_chip(st_part)
        wb_core = [to_core(w) for w in mlp_w]

        norms = tuple(v.reshape(1, -1) for v in (ln1_gain, ln1_bias, ln2_gain, ln2_bias))
        common = (x_in, norms, *rope_tables(start_pos, chunk_len, key_dim))
        all_seqs, pair_seqs, one = (SEQ, SEQ + 1, SEQ + 2), (SEQ + 1, SEQ + 2), (SEQ,)

        z_own_single, new_own_single = run(meta, common, one, one, (0,), (own,), (head_places(head_w),))
        z_own_single, wa_part = lax.optimization_barrier((z_own_single, wa_part))
        wa_quarters = gather(wa_part)
        z_own, new_states = run(meta, common, pair_seqs, pair_seqs, (0,), (own,), (head_places(head_w),), pair=True)
        z_own, wa_core, s_core, wb_part = lax.optimization_barrier((z_own, wa_core, s_core, wb_part))
        wb_quarters = gather(wb_part)
        z_core, new_core = run(meta, common, all_seqs, all_seqs, (1,), (s_core,), (head_places(wa_core),))
        z_core, wa_quarters, wb_quarters, su_chip = lax.optimization_barrier((z_core, wa_quarters, wb_quarters, su_chip))
        wa_far, wb_far, su_far = [to_core(w) for w in wa_quarters], [to_core(w) for w in wb_quarters], to_core(su_chip)
        got_core = to_core(new_core)

        w_chip = heads_gathered(wa_quarters)
        z_chip, new_chip = run(meta, common, one, (STATE_SINGLE,), (2,), (su_chip,), (w_chip,))
        z_chip, wa_far, wb_far, wb_core, su_far, st_chip = lax.optimization_barrier((z_chip, wa_far, wb_far, wb_core, su_far, st_chip))
        st_far = to_core(st_chip)
        w_far = heads_gathered(wa_far)
        mlp = (mlp_places(mlp_w), mlp_places(wb_core), heads_gathered(wb_quarters), heads_gathered(wb_far))
        whole, x_single, new_far = run(meta, common, one, (STATE_SINGLE,), (3,), (su_far,), (w_far, *mlp), ((z_own_single, 0), (z_core, 0), (z_chip, 0)))
        x_single_chip = to_chip(x_single)
        x_single_core = to_core(x_single)
        got_chip = to_chip(new_chip)
        got_far = to_far(new_far)
        whole, x_a, x_b, _, _ = run(meta, common, pair_seqs, (STATE_TWICE, STATE_TWICE + 1), (2, 3), (st_chip, st_far), (w_chip, w_far, *mlp),
                                    ((z_own, 0), (z_core, 1)), whole)
        x_a_core = to_core(x_a)
        x_single_far = to_core(x_single_chip)

        x_b_core = to_core(x_b)

        single_o, twice_o = 2 * chip + other, 4 + 2 * other
        far_c, far_o = 2 * (1 - chip) + core, 2 * (1 - chip) + other
        ids = jnp.stack([single_o, far_c, single, single_o, twice_o, twice_o + 1, far_c, far_o, twice_o, far_o, twice_o + 1]).astype(jnp.int32)
        cuts = chunk_len // TILE
        near = [(x_single_core, 0, 0, cuts), (x_single_chip, 0, 0, cuts)]
        near += [(arr, at, 1, 1) for arr, at in ((new_own_single, 0), (got_core, 0), (got_core, 1), (got_core, 2), (got_chip, 0), (got_far, 0))]
        whole, new_states = place(ids[:8], near, (whole, new_states))
        whole, = place(ids[8:9], [(x_a_core, 0, 0, cuts)], (whole,))
        whole, = place(ids[9:10], [(x_single_far, 0, 0, cuts)], (whole,))
        whole, = place(ids[10:], [(x_b_core, 0, 0, cuts)], (whole,))
        return whole, new_states[:, None]

    in_specs = (P("dp", None, None), P("dp"), P("dp", "tp", None, None), P(), P(), P(None, "tp"), P(None, "tp"), P(None, "tp"), P(None, "tp"), P("tp", None), P(), P(), P(None, "tp"), P("tp", None))
    out_specs = (P("dp", None, None), P("dp", "tp", None, None))
    return jax.shard_map(local_layer, mesh=mesh, in_specs=in_specs, out_specs=out_specs, check_vma=False)
```

```python
import functools

import jax
import jax.numpy as jnp
import numpy as np
from jax import lax
from jax.experimental import pallas as pl
from jax.experimental.pallas import tpu as pltpu
from jax.sharding import PartitionSpec as P


NORM_EPS = 1e-5
GROUP_EPS = 1e-6
ROPE_BASE = 10000.0
TILE = 256
NUM_HEADS = 4
LOG_GAMMA = [float(np.log1p(-np.exp2(-5.0 - n))) for n in range(NUM_HEADS)]
SEQ, STATE_SINGLE, STATE_TWICE, GROUP, HEAD, PAIR, OTHER_CHIP = 0, 3, 4, 6, 7, 8, 9
BF16 = jnp.bfloat16
F32 = jnp.float32
ANY = pl.BlockSpec(memory_space=pl.ANY)


def dot(a, b):
    return jnp.dot(a, b, preferred_element_type=F32)


def layer_norm(x_f32, norm_gain, norm_bias):
    row_mean = jnp.mean(x_f32, axis=-1, keepdims=True)
    centered = x_f32 - row_mean
    variance = jnp.mean(centered * centered, axis=-1, keepdims=True)
    return centered * lax.rsqrt(variance + NORM_EPS) * norm_gain + norm_bias


def rotate(v, cos_t, sin_t):
    half = v.shape[-1] // 2
    a, b = v[:, :half], v[:, half:]
    return jnp.concatenate([a * cos_t - b * sin_t, b * cos_t + a * sin_t], axis=-1)


def widen(row_table, width):
    return jnp.concatenate([row_table] * (width // row_table.shape[-1]), axis=-1)


def log_decay(head):
    value = jnp.float32(LOG_GAMMA[0])
    for n, log_gamma in enumerate(LOG_GAMMA[1:], 1):
        value = jnp.where(head == n, jnp.float32(log_gamma), value)
    return value


def fill_decays(log_gammas, inner_ref, rows_ref):
    gap = lax.broadcasted_iota(jnp.int32, (TILE, TILE), 0) - lax.broadcasted_iota(jnp.int32, (TILE, TILE), 1)
    row = lax.broadcasted_iota(jnp.int32, (TILE, 128), 0)
    for i, log_gamma in enumerate(log_gammas):
        inner_ref[i] = jnp.where(gap >= 0, jnp.exp(jnp.maximum(gap, 0).astype(F32) * log_gamma), 0.0)
        rows_ref[i, 0] = jnp.exp((row + 1).astype(F32) * log_gamma)
        rows_ref[i, 1] = jnp.exp((TILE - 1 - row).astype(F32) * log_gamma)
        rows_ref[i, 2] = jnp.exp(jnp.full((TILE, 128), TILE, F32) * log_gamma)


def head_blocks(h, w_ref, state_ref, inner, rows_ref, tables):
    n_seqs, key_dim, val_dim = state_ref.shape
    q_raw = dot(h, w_ref[:, :key_dim])
    k_raw = dot(h, w_ref[:, key_dim:2 * key_dim])
    values = dot(h, w_ref[:, 2 * key_dim:2 * key_dim + val_dim]).astype(BF16)
    gates = dot(h, w_ref[:, 2 * key_dim + val_dim:])
    out = []
    for i, table in enumerate(tables):
        at, b = slice(i * TILE, (i + 1) * TILE), i * n_seqs // len(tables)
        queries = rotate(q_raw[at], *table).astype(BF16)
        keys = (rotate(k_raw[at], *table) * key_dim ** -0.5).astype(BF16)
        scores = lax.dot_general(queries, keys, (((1,), (1,)), ((), ())), preferred_element_type=F32) * inner
        state = state_ref[b]
        carried = dot(queries, state.astype(BF16)) * widen(rows_ref[0], val_dim)
        retained = dot(scores.astype(BF16), values[at]) + carried
        faded = (keys.astype(F32) * widen(rows_ref[1], key_dim)).astype(BF16)
        update = lax.dot_general(faded, values[at], (((0,), (0,)), ((), ())), preferred_element_type=F32)
        state_ref[b] = state * widen(rows_ref[2, 0:1], val_dim) + update
        row_mean = jnp.mean(retained, axis=-1, keepdims=True)
        centered = retained - row_mean
        variance = jnp.mean(centered * centered, axis=-1, keepdims=True)
        normed = centered * lax.rsqrt(variance + GROUP_EPS)
        out.append((gates[at] * lax.logistic(gates[at]) * normed).astype(BF16))
    return out


def kernel_body(n_seqs, n_sub, heads, n_z, pieces, with_whole, meta_ref, gain1, bias1, gain2, bias2, step_ref, *refs):
    it = iter(refs)

    def take(n):
        return [next(it) for _ in range(n)]

    x_refs, base_refs, s_refs, z_refs = take(n_seqs), take(n_seqs), [take(n_seqs) for _ in heads], [take(n_seqs) for _ in range(n_z)]
    sources = [take(len(p)) for p in pieces]
    take(with_whole)
    outs = take(1 + n_seqs if n_z else 1)
    state_refs = take(len(heads))
    inner_ref, rows_ref, sem = take(3)
    weights = take(len(pieces))

    @pl.when(pl.program_id(0) == 0)
    def _():
        copies = []
        for w_ref, refs_in, places in zip(weights, sources, pieces):
            for ref, (row, col, flip) in zip(refs_in, places):
                if flip is not None:
                    row = pl.multiple_of((meta_ref[GROUP] ^ flip) * ref.shape[0], 256)
                dst = w_ref.at[pl.ds(row, ref.shape[0]), pl.ds(col, ref.shape[1])]
                copies.append(pltpu.make_async_copy(ref, dst, sem.at[len(copies)]))
                copies[-1].start()
        fill_decays([log_decay(meta_ref[HEAD] ^ head) for head in heads], inner_ref, rows_ref)
        for per_head, state_ref in zip(s_refs, state_refs):
            for b, s_ref in enumerate(per_head):
                state_ref[b] = s_ref[0]
        for copy in copies:
            copy.wait()

    cos_b, sin_b = step_ref[0], step_ref[1]
    normed, tables = [], []
    for x_ref, base_ref in zip(x_refs, base_refs):
        normed.append(layer_norm(x_ref[0].astype(F32), gain1[...], bias1[...]).astype(BF16))
        for j in range(n_sub):
            at = pl.multiple_of((pl.program_id(0) * n_sub + j) * 8, 8)
            cos_a, sin_a = base_ref[0, pl.ds(at, 1), :], base_ref[0, pl.ds(at + 1, 1), :]
            tables.append((cos_a * cos_b - sin_a * sin_b, sin_a * cos_b + cos_a * sin_b))
    h = below(normed)
    mixed = [head_blocks(h, weights[i], state_refs[i], inner_ref[i], rows_ref.at[i], tables) for i in range(len(heads))]
    rows = n_sub * TILE
    if not n_z:
        for i, block in enumerate(mixed[0]):
            outs[0][i // n_sub, i % n_sub * TILE:(i % n_sub + 1) * TILE] = block
        return
    mixed = [[ref[0] for ref in refs_of] for refs_of in z_refs] + mixed
    blocks = weights[len(heads):]
    val_dim, d_model = mixed[0][0].shape[1], x_refs[0].shape[2]
    u = sum(dot(below(z), wb[:val_dim, :d_model]) for z, wb in zip(mixed, blocks))
    x_mid = (below([x_ref[0] for x_ref in x_refs]).astype(F32) + u.astype(BF16).astype(F32)).astype(BF16)
    h_two = layer_norm(x_mid.astype(F32), gain2[...], bias2[...]).astype(BF16)
    f = jnp.zeros(u.shape, F32)
    for wb in blocks:
        up = dot(h_two, wb[:, d_model:])
        act = (up * 0.5 * (1.0 + lax.erf(up * 0.5 ** 0.5))).astype(BF16)
        f = f + dot(act, wb[val_dim:, :d_model])
    x_out = (x_mid.astype(F32) + f.astype(BF16).astype(F32)).astype(BF16)
    for b in range(n_seqs):
        outs[0][b] = x_out[b * rows:(b + 1) * rows]
        outs[1 + b][0] = x_out[b * rows:(b + 1) * rows]


def below(blocks):
    return blocks[0] if len(blocks) == 1 else jnp.concatenate(blocks, axis=0)


def run(meta, common, seqs, state_rows, heads, states, weights, zs=(), whole=None, pair=False, n_sub=1):
    x, norms, base, step = common
    tile = n_sub * TILE
    n, chunk_len, d_model = len(seqs), x.shape[1], x.shape[2]
    key_dim, val_dim = states[0].shape[1:]

    def row_spec(shape, at):
        return pl.BlockSpec((1,) + shape, lambda t, m: (m[at], 0, 0))

    def token_spec(at):
        return pl.BlockSpec((1, tile, d_model), lambda t, m: (m[at], t, 0))

    def tile_of(width, count=1, at=0):
        return pl.BlockSpec((count, tile, width), lambda t, m: (at, t, 0))

    def resident(arr):
        return pl.BlockSpec(arr.shape, lambda t, m: (0,) * arr.ndim, pipeline_mode=pl.Buffered(1))

    specs = [resident(arr) for arr in (*norms, step)] + [token_spec(at) for at in seqs] + [row_spec(base.shape[1:], at) for at in seqs]
    args = [*norms, step] + [x] * n + [base] * n
    for state in states:
        specs += [row_spec(state.shape[1:], at) for at in state_rows]
        args += [state] * n
    for z, first in zs:
        specs += [tile_of(val_dim, 1, first + b) for b in range(n)]
        args += [z] * n
    pieces = []
    for weight in weights:
        pieces.append(tuple(place for _, place in weight))
        args += [arr for arr, _ in weight]
        specs += [ANY] * len(weight)
    aliases = {}
    if whole is not None:
        aliases = {len(args) + 1: 0}
        args.append(whole)
        specs.append(ANY)
    if zs:
        whole_spec = token_spec(seqs[0]) if n == 1 else pl.BlockSpec((n, tile, d_model), lambda t, m: (m[PAIR], t, 0))
        outs = [(whole_spec, jax.ShapeDtypeStruct(x.shape, BF16))] + [(tile_of(d_model), jax.ShapeDtypeStruct((1, chunk_len, d_model), BF16))] * n
    else:
        outs = [(tile_of(val_dim, n), jax.ShapeDtypeStruct((n, chunk_len, val_dim), BF16))]
    state_out = pl.BlockSpec((n, key_dim, val_dim), lambda t, m: (m[PAIR] if pair else 0, 0, 0))
    outs += [(state_out, jax.ShapeDtypeStruct((x.shape[0] if pair else n, key_dim, val_dim), F32))] * len(heads)
    flops = n * len(heads) * 2 * (d_model * (2 * key_dim + 2 * val_dim) + TILE * (key_dim + val_dim) + 2 * key_dim * val_dim)
    flops += n * 24 * d_model * val_dim if zs else 0
    return pl.pallas_call(
        functools.partial(kernel_body, n, n_sub, tuple(heads), len(zs), tuple(pieces), whole is not None),
        grid_spec=pltpu.PrefetchScalarGridSpec(
            num_scalar_prefetch=1, grid=(chunk_len // tile,), in_specs=specs, out_specs=[spec for spec, _ in outs],
            scratch_shapes=[pltpu.VMEM((len(heads), TILE, TILE), F32), pltpu.VMEM((len(heads), 3, TILE, 128), F32), pltpu.SemaphoreType.DMA((sum(map(len, pieces)),))]
            + [pltpu.VMEM((d_model, 2 * key_dim + 2 * val_dim), BF16) for _ in weights]),
        out_shape=[shape for _, shape in outs],
        compiler_params=pltpu.CompilerParams(dimension_semantics=("arbitrary",), vmem_limit_bytes=58 << 20),
        cost_estimate=pl.CostEstimate(flops=chunk_len * flops, bytes_accessed=n * chunk_len * d_model * (8 if zs else 4), transcendentals=0),
        input_output_aliases=aliases,
        name="tail" if zs else "heads",
    )(meta, *args)


def parts_kernel(meta_ref, w_q, w_k, w_v, w_g, w_o, w_down, w_up, own, heads_out, mlp_out, single_out, twice_out, heads_buf, mlp_buf, single_buf, twice_buf, sem, sem_out):
    rows, group = heads_buf.shape[0], meta_ref[GROUP]
    at = pl.ds(pl.multiple_of(group * rows, rows), rows)
    half = pl.ds(pl.multiple_of((group % 2) * rows, rows), rows)
    d_model = w_o.shape[1]
    copies, col = [], 0
    for w in (w_q, w_k, w_v, w_g):
        copies.append(pltpu.make_async_copy(w.at[at], heads_buf.at[:, pl.ds(col, w.shape[1])], sem.at[len(copies)]))
        col += w.shape[1]
    copies.append(pltpu.make_async_copy(w_up.at[at], mlp_buf.at[:, pl.ds(d_model, w_up.shape[1])], sem.at[len(copies)]))
    copies.append(pltpu.make_async_copy(own.at[pl.ds(meta_ref[OTHER_CHIP], 2)], single_buf, sem.at[len(copies)]))
    copies.append(pltpu.make_async_copy(own.at[pl.ds(4, 4)], twice_buf, sem.at[len(copies)]))
    last = [pltpu.make_async_copy(w.at[half], mlp_buf.at[:, pl.ds(0, d_model)], sem.at[len(copies)]) for w in (w_o, w_down)]
    for copy in copies[:5]:
        copy.start()

    @pl.when(group < 2)
    def _():
        last[0].start()

    @pl.when(group >= 2)
    def _():
        last[1].start()

    for copy in copies[5:]:
        copy.start()
    pushes = [pltpu.make_async_copy(buf, out, sem_out.at[i]) for i, (buf, out) in
              enumerate(((heads_buf, heads_out), (mlp_buf, mlp_out), (single_buf, single_out), (twice_buf, twice_out)))]
    for push, pulls in zip(pushes, (copies[:4], [copies[4], last[0]], copies[5:6], copies[6:])):
        for pull in pulls:
            pull.wait()
        push.start()
    for push in pushes:
        push.wait()


def cut_parts(meta, head_w, mlp_w, own):
    n_rows = mlp_w[0].shape[0] // 2
    shapes = [((n_rows, sum(w.shape[1] for w in head_w)), BF16), ((n_rows, mlp_w[0].shape[1] + mlp_w[2].shape[1]), BF16), ((2,) + own.shape[1:], F32), ((4,) + own.shape[1:], F32)]
    return pl.pallas_call(
        parts_kernel,
        grid_spec=pltpu.PrefetchScalarGridSpec(num_scalar_prefetch=1, grid=(), in_specs=[ANY] * 8, out_specs=[ANY] * 4,
                                               scratch_shapes=[pltpu.VMEM(*shape) for shape in shapes] + [pltpu.SemaphoreType.DMA((8,)), pltpu.SemaphoreType.DMA((4,))]),
        out_shape=[jax.ShapeDtypeStruct(shape, dtype) for shape, dtype in shapes],
        name="parts",
    )(meta, *head_w, *mlp_w, own)


def place_kernel(sources, n_wholes, ids_ref, *refs):
    in_refs, out_refs = refs[:len(sources)], refs[len(sources) + n_wholes:len(sources) + 2 * n_wholes]
    bufs, sem_in, sem_out = refs[len(sources) + 2 * n_wholes:-2], refs[-2], refs[-1]
    pulls, pushes, k = [], [], 0
    for i, ((seq, target, cuts), ref, buf) in enumerate(zip(sources, in_refs, bufs)):
        rows = buf.shape[0] // cuts
        for c in range(cuts):
            part = pl.ds(c * rows, rows)
            pulls.append(pltpu.make_async_copy(ref.at[seq, part], buf.at[part], sem_in.at[k]))
            pushes.append(pltpu.make_async_copy(buf.at[part], out_refs[target].at[ids_ref[i], part], sem_out.at[k]))
            k += 1
    for pull in pulls:
        pull.start()
    for pull, push in zip(pulls, pushes):
        pull.wait()
        push.start()
    for push in pushes:
        push.wait()


def place(ids, blocks, wholes):
    n, n_copies = len(blocks), sum(cuts for *_, cuts in blocks)
    return pl.pallas_call(
        functools.partial(place_kernel, tuple(block[1:] for block in blocks), len(wholes)),
        grid_spec=pltpu.PrefetchScalarGridSpec(
            num_scalar_prefetch=1, grid=(), in_specs=[ANY] * (n + len(wholes)), out_specs=[ANY] * len(wholes),
            scratch_shapes=[pltpu.VMEM(arr.shape[1:], arr.dtype) for arr, *_ in blocks] + [pltpu.SemaphoreType.DMA((n_copies,))] * 2),
        out_shape=[jax.ShapeDtypeStruct(arr.shape, arr.dtype) for arr in wholes],
        compiler_params=pltpu.CompilerParams(vmem_limit_bytes=40 << 20),
        input_output_aliases={1 + n + i: i for i in range(len(wholes))},
        name="place",
    )(ids, *(arr for arr, *_ in blocks), *wholes)


def rope_tables(start_pos, chunk_len, key_dim):
    half_dim = key_dim // 2
    inv_freq = jnp.power(ROPE_BASE, -jnp.arange(half_dim).astype(F32) / half_dim)
    starts = (start_pos[:, None] + jnp.arange(0, chunk_len, TILE)[None, :]).astype(F32)
    base = starts[:, :, None, None] * inv_freq
    row = lax.broadcasted_iota(jnp.int32, (1, 1, 8, 1), 2)
    base = jnp.where(row == 0, jnp.cos(base), jnp.sin(base))
    step = jnp.arange(TILE).astype(F32)[None, :, None] * inv_freq
    kind = lax.broadcasted_iota(jnp.int32, (2, 1, 1), 0)
    return base.reshape(start_pos.shape[0], -1, half_dim), jnp.where(kind == 0, jnp.cos(step), jnp.sin(step))


def solution(mesh):
    n_dp = mesh.shape["dp"]

    def swap(axis, bits):
        return functools.partial(lax.ppermute, axis_name=axis, perm=[(i, i ^ bits) for i in range(mesh.shape[axis])])

    to_core, to_chip, to_far = swap("tp", 1), swap("tp", 2), swap("tp", 3)

    def local_layer(x_in, start_pos, kv_state, ln1_gain, ln1_bias, w_q, w_k, w_v, w_g, w_o, ln2_gain, ln2_bias, w_up, w_down):
        tp, group = lax.axis_index("tp"), lax.axis_index("dp")
        chip, core = tp // 2, tp % 2
        other = 1 - core
        chunk_len, d_model = x_in.shape[1:]
        own = kv_state[:, 0]
        key_dim, val_dim = own.shape[1:]

        def head_places(arrs):
            return [(w, (0, col, None)) for w, col in zip(arrs, (0, key_dim, 2 * key_dim, 2 * key_dim + val_dim))]

        def mlp_places(arrs):
            return [(w, at) for w, at in zip(arrs, ((0, 0, None), (val_dim, 0, None), (0, d_model, None)))]

        def heads_gathered(quarters):
            return [(w, (0, 0, flip)) for flip, w in enumerate(quarters)]

        def gather(part):
            return [part] + [swap("dp", flip)(part) for flip in range(1, n_dp)]

        head_w, mlp_w = (w_q, w_k, w_v, w_g), (w_o, w_down, w_up)
        single, twice = 2 * chip + core, 4 + 2 * core
        meta = jnp.stack([single, twice, twice + 1, core, 2 * core, 2 * core + 1, group, tp, twice // 2, 2 * (1 - chip)]).astype(jnp.int32)
        wa_core = [to_core(w) for w in head_w]
        s_core = to_core(own)
        wa_part, wb_part, su_part, st_part = cut_parts(meta, head_w, mlp_w, own)
        wa_part = to_chip(wa_part)
        wb_part = to_chip(wb_part)
        su_chip = to_chip(su_part)
        st_chip = to_chip(st_part)
        wb_core = [to_core(w) for w in mlp_w]

        norms = tuple(v.reshape(1, -1) for v in (ln1_gain, ln1_bias, ln2_gain, ln2_bias))
        common = (x_in, norms, *rope_tables(start_pos, chunk_len, key_dim))
        all_seqs, pair_seqs, one = (SEQ, SEQ + 1, SEQ + 2), (SEQ + 1, SEQ + 2), (SEQ,)

        z_own_single, new_own_single = run(meta, common, one, one, (0,), (own,), (head_places(head_w),))
        z_own_single, wa_part = lax.optimization_barrier((z_own_single, wa_part))
        wa_quarters = gather(wa_part)
        z_own, new_states = run(meta, common, pair_seqs, pair_seqs, (0,), (own,), (head_places(head_w),), pair=True)
        z_own, wa_core, s_core, wb_part = lax.optimization_barrier((z_own, wa_core, s_core, wb_part))
        wb_quarters = gather(wb_part)
        z_core, new_core = run(meta, common, all_seqs, all_seqs, (1,), (s_core,), (head_places(wa_core),))
        z_core, wa_quarters, wb_quarters, su_chip = lax.optimization_barrier((z_core, wa_quarters, wb_quarters, su_chip))
        wa_far, wb_far, su_far = [to_core(w) for w in wa_quarters], [to_core(w) for w in wb_quarters], to_core(su_chip)
        got_core = to_core(new_core)

        w_chip = heads_gathered(wa_quarters)
        z_chip, new_chip = run(meta, common, one, (STATE_SINGLE,), (2,), (su_chip,), (w_chip,), n_sub=2)
        z_chip, wa_far, wb_far, wb_core, su_far, st_chip = lax.optimization_barrier((z_chip, wa_far, wb_far, wb_core, su_far, st_chip))
        st_far = to_core(st_chip)
        w_far = heads_gathered(wa_far)
        mlp = (mlp_places(mlp_w), mlp_places(wb_core), heads_gathered(wb_quarters), heads_gathered(wb_far))
        whole, x_single, new_far = run(meta, common, one, (STATE_SINGLE,), (3,), (su_far,), (w_far, *mlp), ((z_own_single, 0), (z_core, 0), (z_chip, 0)), n_sub=2)
        x_single_chip = to_chip(x_single)
        x_single_core = to_core(x_single)
        got_chip = to_chip(new_chip)
        got_far = to_far(new_far)
        whole, x_a, x_b, _, _ = run(meta, common, pair_seqs, (STATE_TWICE, STATE_TWICE + 1), (2, 3), (st_chip, st_far), (w_chip, w_far, *mlp),
                                    ((z_own, 0), (z_core, 1)), whole)
        x_a_core = to_core(x_a)
        x_single_far = to_core(x_single_chip)

        x_b_core = to_core(x_b)

        single_o, twice_o = 2 * chip + other, 4 + 2 * other
        far_c, far_o = 2 * (1 - chip) + core, 2 * (1 - chip) + other
        ids = jnp.stack([single_o, far_c, single, single_o, twice_o, twice_o + 1, far_c, far_o, twice_o, far_o, twice_o + 1]).astype(jnp.int32)
        cuts = chunk_len // TILE
        near = [(x_single_core, 0, 0, cuts), (x_single_chip, 0, 0, cuts)]
        near += [(arr, at, 1, 1) for arr, at in ((new_own_single, 0), (got_core, 0), (got_core, 1), (got_core, 2), (got_chip, 0), (got_far, 0))]
        whole, new_states = place(ids[:8], near, (whole, new_states))
        whole, = place(ids[8:9], [(x_a_core, 0, 0, cuts)], (whole,))
        whole, = place(ids[9:10], [(x_single_far, 0, 0, cuts)], (whole,))
        whole, = place(ids[10:], [(x_b_core, 0, 0, cuts)], (whole,))
        return whole, new_states[:, None]

    in_specs = (P("dp", None, None), P("dp"), P("dp", "tp", None, None), P(), P(), P(None, "tp"), P(None, "tp"), P(None, "tp"), P(None, "tp"), P("tp", None), P(), P(), P(None, "tp"), P("tp", None))
    out_specs = (P("dp", None, None), P("dp", "tp", None, None))
    return jax.shard_map(local_layer, mesh=mesh, in_specs=in_specs, out_specs=out_specs, check_vma=False)
```

```python
import functools

import jax
import jax.numpy as jnp
import numpy as np
from jax import lax
from jax.experimental import pallas as pl
from jax.experimental.pallas import tpu as pltpu
from jax.sharding import PartitionSpec as P


NORM_EPS = 1e-5
GROUP_EPS = 1e-6
ROPE_BASE = 10000.0
TILE = 256
NUM_HEADS = 4
LOG_GAMMA = [float(np.log1p(-np.exp2(-5.0 - n))) for n in range(NUM_HEADS)]
SEQ, STATE_SINGLE, STATE_TWICE, GROUP, HEAD, PAIR, OTHER_CHIP = 0, 3, 4, 6, 7, 8, 9
BF16 = jnp.bfloat16
F32 = jnp.float32
ANY = pl.BlockSpec(memory_space=pl.ANY)


def dot(a, b):
    return jnp.dot(a, b, preferred_element_type=F32)


def layer_norm(x_f32, norm_gain, norm_bias):
    row_mean = jnp.mean(x_f32, axis=-1, keepdims=True)
    centered = x_f32 - row_mean
    variance = jnp.mean(centered * centered, axis=-1, keepdims=True)
    return centered * lax.rsqrt(variance + NORM_EPS) * norm_gain + norm_bias


def rotate(v, cos_t, sin_t):
    half = v.shape[-1] // 2
    a, b = v[:, :half], v[:, half:]
    return jnp.concatenate([a * cos_t - b * sin_t, b * cos_t + a * sin_t], axis=-1)


def widen(row_table, width):
    return jnp.concatenate([row_table] * (width // row_table.shape[-1]), axis=-1)


def log_decay(head):
    value = jnp.float32(LOG_GAMMA[0])
    for n, log_gamma in enumerate(LOG_GAMMA[1:], 1):
        value = jnp.where(head == n, jnp.float32(log_gamma), value)
    return value


def fill_decays(log_gammas, inner_ref, rows_ref):
    gap = lax.broadcasted_iota(jnp.int32, (TILE, TILE), 0) - lax.broadcasted_iota(jnp.int32, (TILE, TILE), 1)
    row = lax.broadcasted_iota(jnp.int32, (TILE, 128), 0)
    for i, log_gamma in enumerate(log_gammas):
        inner_ref[i] = jnp.where(gap >= 0, jnp.exp(jnp.maximum(gap, 0).astype(F32) * log_gamma), 0.0)
        rows_ref[i, 0] = jnp.exp((row + 1).astype(F32) * log_gamma)
        rows_ref[i, 1] = jnp.exp((TILE - 1 - row).astype(F32) * log_gamma)
        rows_ref[i, 2] = jnp.exp(jnp.full((TILE, 128), TILE, F32) * log_gamma)


def head_blocks(hs, w_ref, state_ref, inner, rows_ref, tables):
    n_seqs, key_dim, val_dim = state_ref.shape
    out = []
    for i, (h, table) in enumerate(zip(hs, tables)):
        b = i * n_seqs // len(tables)
        q_raw = dot(h, w_ref[:, :key_dim])
        k_raw = dot(h, w_ref[:, key_dim:2 * key_dim])
        queries = rotate(q_raw, *table).astype(BF16)
        keys = (rotate(k_raw, *table) * key_dim ** -0.5).astype(BF16)
        values = dot(h, w_ref[:, 2 * key_dim:2 * key_dim + val_dim]).astype(BF16)
        scores = lax.dot_general(queries, keys, (((1,), (1,)), ((), ())), preferred_element_type=F32) * inner
        state = state_ref[b]
        carried = dot(queries, state.astype(BF16)) * widen(rows_ref[0], val_dim)
        retained = dot(scores.astype(BF16), values) + carried
        gates = dot(h, w_ref[:, 2 * key_dim + val_dim:])
        faded = (keys.astype(F32) * widen(rows_ref[1], key_dim)).astype(BF16)
        update = lax.dot_general(faded, values, (((0,), (0,)), ((), ())), preferred_element_type=F32)
        state_ref[b] = state * widen(rows_ref[2, 0:1], val_dim) + update
        row_mean = jnp.mean(retained, axis=-1, keepdims=True)
        centered = retained - row_mean
        variance = jnp.mean(centered * centered, axis=-1, keepdims=True)
        normed = centered * lax.rsqrt(variance + GROUP_EPS)
        out.append((gates * lax.logistic(gates) * normed).astype(BF16))
    return out


def kernel_body(n_seqs, n_sub, heads, n_z, pieces, with_whole, meta_ref, gain1, bias1, gain2, bias2, step_ref, *refs):
    it = iter(refs)

    def take(n):
        return [next(it) for _ in range(n)]

    x_refs, base_refs, s_refs, z_refs = take(n_seqs), take(n_seqs), [take(n_seqs) for _ in heads], [take(n_seqs) for _ in range(n_z)]
    sources = take(len(pieces))
    take(with_whole)
    outs = take(1 + n_seqs if n_z else 1)
    state_refs = take(len(heads))
    inner_ref, rows_ref, sem = take(3)
    weights = list(it)

    @pl.when(pl.program_id(0) == 0)
    def _():
        copies = []
        for ref, cuts in zip(sources, pieces):
            for to, row, col, first, width, flip, skip in cuts:
                if flip is not None:
                    quarter = meta_ref[GROUP] ^ flip
                    row = pl.multiple_of(row + quarter * ref.shape[0] + quarter // 2 * skip, 256)
                dst = weights[to].at[pl.ds(row, ref.shape[0]), pl.ds(col, width)]
                copies.append(pltpu.make_async_copy(ref.at[:, pl.ds(first, width)], dst, sem.at[len(copies)]))
                copies[-1].start()
        fill_decays([log_decay(meta_ref[HEAD] ^ head) for head in heads], inner_ref, rows_ref)
        for per_head, state_ref in zip(s_refs, state_refs):
            for b, s_ref in enumerate(per_head):
                state_ref[b] = s_ref[0]
        for copy in copies:
            copy.wait()

    cos_b, sin_b = step_ref[0], step_ref[1]
    normed, tables = [], []
    for x_ref, base_ref in zip(x_refs, base_refs):
        normed.append(layer_norm(x_ref[0].astype(F32), gain1[...], bias1[...]).astype(BF16))
        for j in range(n_sub):
            at = pl.multiple_of((pl.program_id(0) * n_sub + j) * 8, 8)
            cos_a, sin_a = base_ref[0, pl.ds(at, 1), :], base_ref[0, pl.ds(at + 1, 1), :]
            tables.append((cos_a * cos_b - sin_a * sin_b, sin_a * cos_b + cos_a * sin_b))
    hs = [h[j * TILE:(j + 1) * TILE] for h in normed for j in range(n_sub)]
    mixed = [head_blocks(hs, weights[i], state_refs[i], inner_ref[i], rows_ref.at[i], tables) for i in range(len(heads))]
    rows = n_sub * TILE
    if not n_z:
        for i, block in enumerate(mixed[0]):
            outs[0][i // n_sub, i % n_sub * TILE:(i % n_sub + 1) * TILE] = block
        return
    mixed = [[ref[0] for ref in refs_of] for refs_of in z_refs] + mixed
    w_od, w_up = weights[len(heads):]
    width = w_up.shape[1]
    u = dot(jnp.concatenate([below(z) for z in mixed], axis=1), w_od[:width])
    x_mid = (below([x_ref[0] for x_ref in x_refs]).astype(F32) + u.astype(BF16).astype(F32)).astype(BF16)
    h_two = layer_norm(x_mid.astype(F32), gain2[...], bias2[...]).astype(BF16)
    acts = []
    for at in range(0, width, width // 4):
        up = dot(h_two, w_up[:, at:at + width // 4])
        acts.append((up * 0.5 * (1.0 + lax.erf(up * 0.5 ** 0.5))).astype(BF16))
    f = dot(jnp.concatenate(acts, axis=1), w_od[width:])
    x_out = (x_mid.astype(F32) + f.astype(BF16).astype(F32)).astype(BF16)
    for b in range(n_seqs):
        outs[0][b] = x_out[b * rows:(b + 1) * rows]
        outs[1 + b][0] = x_out[b * rows:(b + 1) * rows]


def below(blocks):
    return blocks[0] if len(blocks) == 1 else jnp.concatenate(blocks, axis=0)


def run(meta, common, seqs, state_rows, heads, states, weights, zs=(), whole=None, pair=False, n_sub=1):
    x, norms, base, step = common
    tile = n_sub * TILE
    n, chunk_len, d_model = len(seqs), x.shape[1], x.shape[2]
    key_dim, val_dim = states[0].shape[1:]

    def row_spec(shape, at):
        return pl.BlockSpec((1,) + shape, lambda t, m: (m[at], 0, 0))

    def token_spec(at):
        return pl.BlockSpec((1, tile, d_model), lambda t, m: (m[at], t, 0))

    def tile_of(width, count=1, at=0):
        return pl.BlockSpec((count, tile, width), lambda t, m: (at, t, 0))

    def resident(arr):
        return pl.BlockSpec(arr.shape, lambda t, m: (0,) * arr.ndim, pipeline_mode=pl.Buffered(1))

    specs = [resident(arr) for arr in (*norms, step)] + [token_spec(at) for at in seqs] + [row_spec(base.shape[1:], at) for at in seqs]
    args = [*norms, step] + [x] * n + [base] * n
    for state in states:
        specs += [row_spec(state.shape[1:], at) for at in state_rows]
        args += [state] * n
    for z, first in zs:
        specs += [tile_of(val_dim, 1, first + b) for b in range(n)]
        args += [z] * n
    pieces = [cuts for _, cuts in weights]
    args += [arr for arr, _ in weights]
    specs += [ANY] * len(weights)
    scratch = [(d_model, 2 * key_dim + 2 * val_dim)] * len(heads)
    if zs:
        scratch += [(2 * NUM_HEADS * val_dim, d_model), (d_model, NUM_HEADS * val_dim)]
    aliases = {}
    if whole is not None:
        aliases = {len(args) + 1: 0}
        args.append(whole)
        specs.append(ANY)
    if zs:
        whole_spec = token_spec(seqs[0]) if n == 1 else pl.BlockSpec((n, tile, d_model), lambda t, m: (m[PAIR], t, 0))
        outs = [(whole_spec, jax.ShapeDtypeStruct(x.shape, BF16))] + [(tile_of(d_model), jax.ShapeDtypeStruct((1, chunk_len, d_model), BF16))] * n
    else:
        outs = [(tile_of(val_dim, n), jax.ShapeDtypeStruct((n, chunk_len, val_dim), BF16))]
    state_out = pl.BlockSpec((n, key_dim, val_dim), lambda t, m: (m[PAIR] if pair else 0, 0, 0))
    outs += [(state_out, jax.ShapeDtypeStruct((x.shape[0] if pair else n, key_dim, val_dim), F32))] * len(heads)
    flops = n * len(heads) * 2 * (d_model * (2 * key_dim + 2 * val_dim) + TILE * (key_dim + val_dim) + 2 * key_dim * val_dim)
    flops += n * 24 * d_model * val_dim if zs else 0
    return pl.pallas_call(
        functools.partial(kernel_body, n, n_sub, tuple(heads), len(zs), tuple(pieces), whole is not None),
        grid_spec=pltpu.PrefetchScalarGridSpec(
            num_scalar_prefetch=1, grid=(chunk_len // tile,), in_specs=specs, out_specs=[spec for spec, _ in outs],
            scratch_shapes=[pltpu.VMEM((len(heads), TILE, TILE), F32), pltpu.VMEM((len(heads), 3, TILE, 128), F32), pltpu.SemaphoreType.DMA((sum(map(len, pieces)),))]
            + [pltpu.VMEM(shape, BF16) for shape in scratch]),
        out_shape=[shape for _, shape in outs],
        compiler_params=pltpu.CompilerParams(dimension_semantics=("arbitrary",), vmem_limit_bytes=58 << 20),
        cost_estimate=pl.CostEstimate(flops=chunk_len * flops, bytes_accessed=n * chunk_len * d_model * (8 if zs else 4), transcendentals=0),
        input_output_aliases=aliases,
        name="tail" if zs else "heads",
    )(meta, *args)


def parts_kernel(meta_ref, w_q, w_k, w_v, w_g, w_o, w_down, w_up, own, heads_out, mlp_out, single_out, twice_out, heads_buf, mlp_buf, single_buf, twice_buf, sem, sem_out):
    rows, group = heads_buf.shape[0], meta_ref[GROUP]
    at = pl.ds(pl.multiple_of(group * rows, rows), rows)
    half = pl.ds(pl.multiple_of((group % 2) * rows, rows), rows)
    d_model = w_o.shape[1]
    copies, col = [], 0
    for w in (w_q, w_k, w_v, w_g):
        copies.append(pltpu.make_async_copy(w.at[at], heads_buf.at[:, pl.ds(col, w.shape[1])], sem.at[len(copies)]))
        col += w.shape[1]
    copies.append(pltpu.make_async_copy(w_up.at[at], mlp_buf.at[:, pl.ds(d_model, w_up.shape[1])], sem.at[len(copies)]))
    copies.append(pltpu.make_async_copy(own.at[pl.ds(meta_ref[OTHER_CHIP], 2)], single_buf, sem.at[len(copies)]))
    copies.append(pltpu.make_async_copy(own.at[pl.ds(4, 4)], twice_buf, sem.at[len(copies)]))
    last = [pltpu.make_async_copy(w.at[half], mlp_buf.at[:, pl.ds(0, d_model)], sem.at[len(copies)]) for w in (w_o, w_down)]
    for copy in copies[:5]:
        copy.start()

    @pl.when(group < 2)
    def _():
        last[0].start()

    @pl.when(group >= 2)
    def _():
        last[1].start()

    for copy in copies[5:]:
        copy.start()
    pushes = [pltpu.make_async_copy(buf, out, sem_out.at[i]) for i, (buf, out) in
              enumerate(((heads_buf, heads_out), (mlp_buf, mlp_out), (single_buf, single_out), (twice_buf, twice_out)))]
    for push, pulls in zip(pushes, (copies[:4], [copies[4], last[0]], copies[5:6], copies[6:])):
        for pull in pulls:
            pull.wait()
        push.start()
    for push in pushes:
        push.wait()


def cut_parts(meta, head_w, mlp_w, own):
    n_rows = mlp_w[0].shape[0] // 2
    shapes = [((n_rows, sum(w.shape[1] for w in head_w)), BF16), ((n_rows, mlp_w[0].shape[1] + mlp_w[2].shape[1]), BF16), ((2,) + own.shape[1:], F32), ((4,) + own.shape[1:], F32)]
    return pl.pallas_call(
        parts_kernel,
        grid_spec=pltpu.PrefetchScalarGridSpec(num_scalar_prefetch=1, grid=(), in_specs=[ANY] * 8, out_specs=[ANY] * 4,
                                               scratch_shapes=[pltpu.VMEM(*shape) for shape in shapes] + [pltpu.SemaphoreType.DMA((8,)), pltpu.SemaphoreType.DMA((4,))]),
        out_shape=[jax.ShapeDtypeStruct(shape, dtype) for shape, dtype in shapes],
        name="parts",
    )(meta, *head_w, *mlp_w, own)


def place_kernel(sources, n_wholes, ids_ref, *refs):
    in_refs, out_refs = refs[:len(sources)], refs[len(sources) + n_wholes:len(sources) + 2 * n_wholes]
    bufs, sem_in, sem_out = refs[len(sources) + 2 * n_wholes:-2], refs[-2], refs[-1]
    pulls, pushes, k = [], [], 0
    for i, ((seq, target, cuts), ref, buf) in enumerate(zip(sources, in_refs, bufs)):
        rows = buf.shape[0] // cuts
        for c in range(cuts):
            part = pl.ds(c * rows, rows)
            pulls.append(pltpu.make_async_copy(ref.at[seq, part], buf.at[part], sem_in.at[k]))
            pushes.append(pltpu.make_async_copy(buf.at[part], out_refs[target].at[ids_ref[i], part], sem_out.at[k]))
            k += 1
    for pull in pulls:
        pull.start()
    for pull, push in zip(pulls, pushes):
        pull.wait()
        push.start()
    for push in pushes:
        push.wait()


def place(ids, blocks, wholes):
    n, n_copies = len(blocks), sum(cuts for *_, cuts in blocks)
    return pl.pallas_call(
        functools.partial(place_kernel, tuple(block[1:] for block in blocks), len(wholes)),
        grid_spec=pltpu.PrefetchScalarGridSpec(
            num_scalar_prefetch=1, grid=(), in_specs=[ANY] * (n + len(wholes)), out_specs=[ANY] * len(wholes),
            scratch_shapes=[pltpu.VMEM(arr.shape[1:], arr.dtype) for arr, *_ in blocks] + [pltpu.SemaphoreType.DMA((n_copies,))] * 2),
        out_shape=[jax.ShapeDtypeStruct(arr.shape, arr.dtype) for arr in wholes],
        compiler_params=pltpu.CompilerParams(vmem_limit_bytes=40 << 20),
        input_output_aliases={1 + n + i: i for i in range(len(wholes))},
        name="place",
    )(ids, *(arr for arr, *_ in blocks), *wholes)


def rope_tables(start_pos, chunk_len, key_dim):
    half_dim = key_dim // 2
    inv_freq = jnp.power(ROPE_BASE, -jnp.arange(half_dim).astype(F32) / half_dim)
    starts = (start_pos[:, None] + jnp.arange(0, chunk_len, TILE)[None, :]).astype(F32)
    base = starts[:, :, None, None] * inv_freq
    row = lax.broadcasted_iota(jnp.int32, (1, 1, 8, 1), 2)
    base = jnp.where(row == 0, jnp.cos(base), jnp.sin(base))
    step = jnp.arange(TILE).astype(F32)[None, :, None] * inv_freq
    kind = lax.broadcasted_iota(jnp.int32, (2, 1, 1), 0)
    return base.reshape(start_pos.shape[0], -1, half_dim), jnp.where(kind == 0, jnp.cos(step), jnp.sin(step))


def solution(mesh):
    n_dp = mesh.shape["dp"]

    def swap(axis, bits):
        return functools.partial(lax.ppermute, axis_name=axis, perm=[(i, i ^ bits) for i in range(mesh.shape[axis])])

    to_core, to_chip, to_far = swap("tp", 1), swap("tp", 2), swap("tp", 3)

    def local_layer(x_in, start_pos, kv_state, ln1_gain, ln1_bias, w_q, w_k, w_v, w_g, w_o, ln2_gain, ln2_bias, w_up, w_down):
        tp, group = lax.axis_index("tp"), lax.axis_index("dp")
        chip, core = tp // 2, tp % 2
        other = 1 - core
        chunk_len, d_model = x_in.shape[1:]
        own = kv_state[:, 0]
        key_dim, val_dim = own.shape[1:]

        def head_places(arrs, to=0):
            return [(w, ((to, 0, col, 0, w.shape[1], None, 0),)) for w, col in zip(arrs, (0, key_dim, 2 * key_dim, 2 * key_dim + val_dim))]

        def heads_gathered(quarters, to=0):
            return [(w, ((to, 0, 0, 0, w.shape[1], flip, 0),)) for flip, w in enumerate(quarters)]

        def mlp_places(arrs, i, to):
            at, down = i * val_dim, NUM_HEADS * val_dim
            return [(w, ((t, row, col, 0, w.shape[1], None, 0),)) for w, (t, row, col) in zip(arrs, ((to, at, 0), (to, down + at, 0), (to + 1, 0, at)))]

        def mlp_gathered(quarters, i, to):
            at, skip = i * val_dim, (NUM_HEADS - 1) * val_dim
            return [(w, ((to, at, 0, 0, d_model, flip, skip), (to + 1, 0, at, d_model, val_dim, flip, 0))) for flip, w in enumerate(quarters)]

        def mlp(to):
            return mlp_places(mlp_w, 0, to) + mlp_places(wb_core, 1, to) + mlp_gathered(wb_quarters, 2, to) + mlp_gathered(wb_far, 3, to)

        def gather(part):
            return [part] + [swap("dp", flip)(part) for flip in range(1, n_dp)]

        head_w, mlp_w = (w_q, w_k, w_v, w_g), (w_o, w_down, w_up)
        single, twice = 2 * chip + core, 4 + 2 * core
        meta = jnp.stack([single, twice, twice + 1, core, 2 * core, 2 * core + 1, group, tp, twice // 2, 2 * (1 - chip)]).astype(jnp.int32)
        wa_core = [to_core(w) for w in head_w]
        s_core = to_core(own)
        wa_part, wb_part, su_part, st_part = cut_parts(meta, head_w, mlp_w, own)
        wa_part = to_chip(wa_part)
        wb_part = to_chip(wb_part)
        su_chip = to_chip(su_part)
        st_chip = to_chip(st_part)
        wb_core = [to_core(w) for w in mlp_w]

        norms = tuple(v.reshape(1, -1) for v in (ln1_gain, ln1_bias, ln2_gain, ln2_bias))
        common = (x_in, norms, *rope_tables(start_pos, chunk_len, key_dim))
        all_seqs, pair_seqs, one = (SEQ, SEQ + 1, SEQ + 2), (SEQ + 1, SEQ + 2), (SEQ,)

        z_own_single, new_own_single = run(meta, common, one, one, (0,), (own,), head_places(head_w))
        z_own_single, wa_part = lax.optimization_barrier((z_own_single, wa_part))
        wa_quarters = gather(wa_part)
        z_own, new_states = run(meta, common, pair_seqs, pair_seqs, (0,), (own,), head_places(head_w), pair=True)
        z_own, wa_core, s_core, wb_part = lax.optimization_barrier((z_own, wa_core, s_core, wb_part))
        wb_quarters = gather(wb_part)
        z_core, new_core = run(meta, common, all_seqs, all_seqs, (1,), (s_core,), head_places(wa_core))
        z_core, wa_quarters, wb_quarters, su_chip = lax.optimization_barrier((z_core, wa_quarters, wb_quarters, su_chip))
        wa_far, wb_far, su_far = [to_core(w) for w in wa_quarters], [to_core(w) for w in wb_quarters], to_core(su_chip)
        got_core = to_core(new_core)

        z_chip, new_chip = run(meta, common, one, (STATE_SINGLE,), (2,), (su_chip,), heads_gathered(wa_quarters))
        z_chip, wa_far, wb_far, wb_core, su_far, st_chip = lax.optimization_barrier((z_chip, wa_far, wb_far, wb_core, su_far, st_chip))
        st_far = to_core(st_chip)
        whole, x_single, new_far = run(meta, common, one, (STATE_SINGLE,), (3,), (su_far,), heads_gathered(wa_far) + mlp(1), ((z_own_single, 0), (z_core, 0), (z_chip, 0)), n_sub=2)
        x_single_chip = to_chip(x_single)
        x_single_core = to_core(x_single)
        got_chip = to_chip(new_chip)
        got_far = to_far(new_far)
        whole, x_a, x_b, _, _ = run(meta, common, pair_seqs, (STATE_TWICE, STATE_TWICE + 1), (2, 3), (st_chip, st_far), heads_gathered(wa_quarters) + heads_gathered(wa_far, 1) + mlp(2),
                                    ((z_own, 0), (z_core, 1)), whole)
        x_a_core = to_core(x_a)
        x_single_far = to_core(x_single_chip)

        x_b_core = to_core(x_b)

        single_o, twice_o = 2 * chip + other, 4 + 2 * other
        far_c, far_o = 2 * (1 - chip) + core, 2 * (1 - chip) + other
        ids = jnp.stack([single_o, far_c, single, single_o, twice_o, twice_o + 1, far_c, far_o, twice_o, far_o, twice_o + 1]).astype(jnp.int32)
        cuts = chunk_len // TILE
        near = [(x_single_core, 0, 0, cuts), (x_single_chip, 0, 0, cuts)]
        near += [(arr, at, 1, 1) for arr, at in ((new_own_single, 0), (got_core, 0), (got_core, 1), (got_core, 2), (got_chip, 0), (got_far, 0))]
        whole, new_states = place(ids[:8], near, (whole, new_states))
        whole, = place(ids[8:9], [(x_a_core, 0, 0, cuts)], (whole,))
        whole, = place(ids[9:10], [(x_single_far, 0, 0, cuts)], (whole,))
        whole, = place(ids[10:], [(x_b_core, 0, 0, cuts)], (whole,))
        return whole, new_states[:, None]

    in_specs = (P("dp", None, None), P("dp"), P("dp", "tp", None, None), P(), P(), P(None, "tp"), P(None, "tp"), P(None, "tp"), P(None, "tp"), P("tp", None), P(), P(), P(None, "tp"), P("tp", None))
    out_specs = (P("dp", None, None), P("dp", "tp", None, None))
    return jax.shard_map(local_layer, mesh=mesh, in_specs=in_specs, out_specs=out_specs, check_vma=False)
```

```python
import functools

import jax
import jax.numpy as jnp
import numpy as np
from jax import lax
from jax.experimental import pallas as pl
from jax.experimental.pallas import tpu as pltpu
from jax.sharding import PartitionSpec as P


NORM_EPS = 1e-5
GROUP_EPS = 1e-6
ROPE_BASE = 10000.0
TILE = 256
NUM_HEADS = 4
LOG_GAMMA = [float(np.log1p(-np.exp2(-5.0 - n))) for n in range(NUM_HEADS)]
SEQ, STATE_SINGLE, STATE_TWICE, GROUP, HEAD, PAIR, OTHER_CHIP = 0, 3, 4, 6, 7, 8, 9
BF16 = jnp.bfloat16
F32 = jnp.float32
ANY = pl.BlockSpec(memory_space=pl.ANY)


def dot(a, b):
    return jnp.dot(a, b, preferred_element_type=F32)


def layer_norm(x_f32, norm_gain, norm_bias):
    row_mean = jnp.mean(x_f32, axis=-1, keepdims=True)
    centered = x_f32 - row_mean
    variance = jnp.mean(centered * centered, axis=-1, keepdims=True)
    return centered * lax.rsqrt(variance + NORM_EPS) * norm_gain + norm_bias


def rotate(v, cos_t, sin_t):
    half = v.shape[-1] // 2
    a, b = v[:, :half], v[:, half:]
    return jnp.concatenate([a * cos_t - b * sin_t, b * cos_t + a * sin_t], axis=-1)


def widen(row_table, width):
    return jnp.concatenate([row_table] * (width // row_table.shape[-1]), axis=-1)


def log_decay(head):
    value = jnp.float32(LOG_GAMMA[0])
    for n, log_gamma in enumerate(LOG_GAMMA[1:], 1):
        value = jnp.where(head == n, jnp.float32(log_gamma), value)
    return value


def fill_decays(log_gammas, inner_ref, rows_ref):
    gap = lax.broadcasted_iota(jnp.int32, (TILE, TILE), 0) - lax.broadcasted_iota(jnp.int32, (TILE, TILE), 1)
    row = lax.broadcasted_iota(jnp.int32, (TILE, 128), 0)
    for i, log_gamma in enumerate(log_gammas):
        inner_ref[i] = jnp.where(gap >= 0, jnp.exp(jnp.maximum(gap, 0).astype(F32) * log_gamma), 0.0)
        rows_ref[i, 0] = jnp.exp((row + 1).astype(F32) * log_gamma)
        rows_ref[i, 1] = jnp.exp((TILE - 1 - row).astype(F32) * log_gamma)
        rows_ref[i, 2] = jnp.exp(jnp.full((TILE, 128), TILE, F32) * log_gamma)


def head_blocks(hs, w_ref, state_ref, inner, rows_ref, tables):
    n_seqs, key_dim, val_dim = state_ref.shape
    out = []
    for i, (h, table) in enumerate(zip(hs, tables)):
        b = i * n_seqs // len(tables)
        q_raw = dot(h, w_ref[:, :key_dim])
        k_raw = dot(h, w_ref[:, key_dim:2 * key_dim])
        queries = rotate(q_raw, *table).astype(BF16)
        keys = (rotate(k_raw, *table) * key_dim ** -0.5).astype(BF16)
        values = dot(h, w_ref[:, 2 * key_dim:2 * key_dim + val_dim]).astype(BF16)
        scores = lax.dot_general(queries, keys, (((1,), (1,)), ((), ())), preferred_element_type=F32) * inner
        state = state_ref[b]
        carried = dot(queries, state.astype(BF16)) * widen(rows_ref[0], val_dim)
        retained = dot(scores.astype(BF16), values) + carried
        gates = dot(h, w_ref[:, 2 * key_dim + val_dim:])
        faded = (keys.astype(F32) * widen(rows_ref[1], key_dim)).astype(BF16)
        update = lax.dot_general(faded, values, (((0,), (0,)), ((), ())), preferred_element_type=F32)
        state_ref[b] = state * widen(rows_ref[2, 0:1], val_dim) + update
        row_mean = jnp.mean(retained, axis=-1, keepdims=True)
        centered = retained - row_mean
        variance = jnp.mean(centered * centered, axis=-1, keepdims=True)
        normed = centered * lax.rsqrt(variance + GROUP_EPS)
        out.append((gates * lax.logistic(gates) * normed).astype(BF16))
    return out


def kernel_body(n_seqs, n_sub, has_h, heads, n_z, pieces, with_whole, meta_ref, gain1, bias1, gain2, bias2, step_ref, *refs):
    it = iter(refs)

    def take(n):
        return [next(it) for _ in range(n)]

    x_refs, h_refs = take(n_seqs if n_z or not has_h else 0), take(n_seqs if has_h else 0)
    base_refs, s_refs, z_refs = take(n_seqs), [take(n_seqs) for _ in heads], [take(n_seqs) for _ in range(n_z)]
    sources = take(len(pieces))
    take(with_whole)
    outs = take(1 + n_seqs if n_z else 1 if has_h else 2)
    state_refs = take(len(heads))
    inner_ref, rows_ref, sem = take(3)
    weights = list(it)

    @pl.when(pl.program_id(0) == 0)
    def _():
        copies = []
        for ref, cuts in zip(sources, pieces):
            for to, row, col, first, width, flip, skip in cuts:
                if flip is not None:
                    quarter = meta_ref[GROUP] ^ flip
                    row = pl.multiple_of(row + quarter * ref.shape[0] + quarter // 2 * skip, 256)
                dst = weights[to].at[pl.ds(row, ref.shape[0]), pl.ds(col, width)]
                copies.append(pltpu.make_async_copy(ref.at[:, pl.ds(first, width)], dst, sem.at[len(copies)]))
                copies[-1].start()
        fill_decays([log_decay(meta_ref[HEAD] ^ head) for head in heads], inner_ref, rows_ref)
        for per_head, state_ref in zip(s_refs, state_refs):
            for b, s_ref in enumerate(per_head):
                state_ref[b] = s_ref[0]
        for copy in copies:
            copy.wait()

    cos_b, sin_b = step_ref[0], step_ref[1]
    tables = []
    for base_ref in base_refs:
        for j in range(n_sub):
            at = pl.multiple_of((pl.program_id(0) * n_sub + j) * 8, 8)
            cos_a, sin_a = base_ref[0, pl.ds(at, 1), :], base_ref[0, pl.ds(at + 1, 1), :]
            tables.append((cos_a * cos_b - sin_a * sin_b, sin_a * cos_b + cos_a * sin_b))
    if has_h:
        normed = [h_ref[0] for h_ref in h_refs]
    else:
        normed = [layer_norm(x_ref[0].astype(F32), gain1[...], bias1[...]).astype(BF16) for x_ref in x_refs]
        for b, h in enumerate(normed):
            outs[1][b] = h
    hs = [h[j * TILE:(j + 1) * TILE] for h in normed for j in range(n_sub)]
    mixed = [head_blocks(hs, weights[i], state_refs[i], inner_ref[i], rows_ref.at[i], tables) for i in range(len(heads))]
    rows = n_sub * TILE
    if not n_z:
        for i, block in enumerate(mixed[0]):
            outs[0][i // n_sub, i % n_sub * TILE:(i % n_sub + 1) * TILE] = block
        return
    mixed = [[ref[0] for ref in refs_of] for refs_of in z_refs] + mixed
    w_od, w_up = weights[len(heads):]
    width = w_up.shape[1]
    u = dot(jnp.concatenate([below(z) for z in mixed], axis=1), w_od[:width])
    x_mid = (below([x_ref[0] for x_ref in x_refs]).astype(F32) + u.astype(BF16).astype(F32)).astype(BF16)
    h_two = layer_norm(x_mid.astype(F32), gain2[...], bias2[...]).astype(BF16)
    acts = []
    for at in range(0, width, width // 4):
        up = dot(h_two, w_up[:, at:at + width // 4])
        acts.append((up * 0.5 * (1.0 + lax.erf(up * 0.5 ** 0.5))).astype(BF16))
    f = dot(jnp.concatenate(acts, axis=1), w_od[width:])
    x_out = (x_mid.astype(F32) + f.astype(BF16).astype(F32)).astype(BF16)
    for b in range(n_seqs):
        outs[0][b] = x_out[b * rows:(b + 1) * rows]
        outs[1 + b][0] = x_out[b * rows:(b + 1) * rows]


def below(blocks):
    return blocks[0] if len(blocks) == 1 else jnp.concatenate(blocks, axis=0)


def run(meta, common, seqs, state_rows, heads, states, weights, zs=(), whole=None, pair=False, n_sub=1, hs=()):
    x, norms, base, step = common
    tile = n_sub * TILE
    n, chunk_len, d_model = len(seqs), x.shape[1], x.shape[2]
    key_dim, val_dim = states[0].shape[1:]

    def row_spec(shape, at):
        return pl.BlockSpec((1,) + shape, lambda t, m: (m[at], 0, 0))

    def token_spec(at):
        return pl.BlockSpec((1, tile, d_model), lambda t, m: (m[at], t, 0))

    def tile_of(width, count=1, at=0):
        return pl.BlockSpec((count, tile, width), lambda t, m: (at, t, 0))

    def resident(arr):
        return pl.BlockSpec(arr.shape, lambda t, m: (0,) * arr.ndim, pipeline_mode=pl.Buffered(1))

    specs, args = [resident(arr) for arr in (*norms, step)], [*norms, step]
    if zs or not hs:
        specs += [token_spec(at) for at in seqs]
        args += [x] * n
    specs += [tile_of(d_model, 1, at) for _, at in hs] + [row_spec(base.shape[1:], at) for at in seqs]
    args += [h for h, _ in hs] + [base] * n
    for state in states:
        specs += [row_spec(state.shape[1:], at) for at in state_rows]
        args += [state] * n
    for z, first in zs:
        specs += [tile_of(val_dim, 1, first + b) for b in range(n)]
        args += [z] * n
    pieces = [cuts for _, cuts in weights]
    args += [arr for arr, _ in weights]
    specs += [ANY] * len(weights)
    scratch = [(d_model, 2 * key_dim + 2 * val_dim)] * len(heads)
    if zs:
        scratch += [(2 * NUM_HEADS * val_dim, d_model), (d_model, NUM_HEADS * val_dim)]
    aliases = {}
    if whole is not None:
        aliases = {len(args) + 1: 0}
        args.append(whole)
        specs.append(ANY)
    if zs:
        whole_spec = token_spec(seqs[0]) if n == 1 else pl.BlockSpec((n, tile, d_model), lambda t, m: (m[PAIR], t, 0))
        outs = [(whole_spec, jax.ShapeDtypeStruct(x.shape, BF16))] + [(tile_of(d_model), jax.ShapeDtypeStruct((1, chunk_len, d_model), BF16))] * n
    else:
        outs = [(tile_of(width, n), jax.ShapeDtypeStruct((n, chunk_len, width), BF16)) for width in ((val_dim,) if hs else (val_dim, d_model))]
    state_out = pl.BlockSpec((n, key_dim, val_dim), lambda t, m: (m[PAIR] if pair else 0, 0, 0))
    outs += [(state_out, jax.ShapeDtypeStruct((x.shape[0] if pair else n, key_dim, val_dim), F32))] * len(heads)
    flops = n * len(heads) * 2 * (d_model * (2 * key_dim + 2 * val_dim) + TILE * (key_dim + val_dim) + 2 * key_dim * val_dim)
    flops += n * 24 * d_model * val_dim if zs else 0
    return pl.pallas_call(
        functools.partial(kernel_body, n, n_sub, bool(hs), tuple(heads), len(zs), tuple(pieces), whole is not None),
        grid_spec=pltpu.PrefetchScalarGridSpec(
            num_scalar_prefetch=1, grid=(chunk_len // tile,), in_specs=specs, out_specs=[spec for spec, _ in outs],
            scratch_shapes=[pltpu.VMEM((len(heads), TILE, TILE), F32), pltpu.VMEM((len(heads), 3, TILE, 128), F32), pltpu.SemaphoreType.DMA((sum(map(len, pieces)),))]
            + [pltpu.VMEM(shape, BF16) for shape in scratch]),
        out_shape=[shape for _, shape in outs],
        compiler_params=pltpu.CompilerParams(dimension_semantics=("arbitrary",), vmem_limit_bytes=58 << 20),
        cost_estimate=pl.CostEstimate(flops=chunk_len * flops, bytes_accessed=n * chunk_len * d_model * (8 if zs else 4), transcendentals=0),
        input_output_aliases=aliases,
        name="tail" if zs else "heads",
    )(meta, *args)


def parts_kernel(meta_ref, w_q, w_k, w_v, w_g, w_o, w_down, w_up, own, heads_out, mlp_out, single_out, twice_out, heads_buf, mlp_buf, single_buf, twice_buf, sem, sem_out):
    rows, group = heads_buf.shape[0], meta_ref[GROUP]
    at = pl.ds(pl.multiple_of(group * rows, rows), rows)
    half = pl.ds(pl.multiple_of((group % 2) * rows, rows), rows)
    d_model = w_o.shape[1]
    copies, col = [], 0
    for w in (w_q, w_k, w_v, w_g):
        copies.append(pltpu.make_async_copy(w.at[at], heads_buf.at[:, pl.ds(col, w.shape[1])], sem.at[len(copies)]))
        col += w.shape[1]
    copies.append(pltpu.make_async_copy(w_up.at[at], mlp_buf.at[:, pl.ds(d_model, w_up.shape[1])], sem.at[len(copies)]))
    copies.append(pltpu.make_async_copy(own.at[pl.ds(meta_ref[OTHER_CHIP], 2)], single_buf, sem.at[len(copies)]))
    copies.append(pltpu.make_async_copy(own.at[pl.ds(4, 4)], twice_buf, sem.at[len(copies)]))
    last = [pltpu.make_async_copy(w.at[half], mlp_buf.at[:, pl.ds(0, d_model)], sem.at[len(copies)]) for w in (w_o, w_down)]
    for copy in copies[:5]:
        copy.start()

    @pl.when(group < 2)
    def _():
        last[0].start()

    @pl.when(group >= 2)
    def _():
        last[1].start()

    for copy in copies[5:]:
        copy.start()
    pushes = [pltpu.make_async_copy(buf, out, sem_out.at[i]) for i, (buf, out) in
              enumerate(((heads_buf, heads_out), (mlp_buf, mlp_out), (single_buf, single_out), (twice_buf, twice_out)))]
    for push, pulls in zip(pushes, (copies[:4], [copies[4], last[0]], copies[5:6], copies[6:])):
        for pull in pulls:
            pull.wait()
        push.start()
    for push in pushes:
        push.wait()


def cut_parts(meta, head_w, mlp_w, own):
    n_rows = mlp_w[0].shape[0] // 2
    shapes = [((n_rows, sum(w.shape[1] for w in head_w)), BF16), ((n_rows, mlp_w[0].shape[1] + mlp_w[2].shape[1]), BF16), ((2,) + own.shape[1:], F32), ((4,) + own.shape[1:], F32)]
    return pl.pallas_call(
        parts_kernel,
        grid_spec=pltpu.PrefetchScalarGridSpec(num_scalar_prefetch=1, grid=(), in_specs=[ANY] * 8, out_specs=[ANY] * 4,
                                               scratch_shapes=[pltpu.VMEM(*shape) for shape in shapes] + [pltpu.SemaphoreType.DMA((8,)), pltpu.SemaphoreType.DMA((4,))]),
        out_shape=[jax.ShapeDtypeStruct(shape, dtype) for shape, dtype in shapes],
        name="parts",
    )(meta, *head_w, *mlp_w, own)


def place_kernel(sources, n_wholes, ids_ref, *refs):
    in_refs, out_refs = refs[:len(sources)], refs[len(sources) + n_wholes:len(sources) + 2 * n_wholes]
    bufs, sem_in, sem_out = refs[len(sources) + 2 * n_wholes:-2], refs[-2], refs[-1]
    pulls, pushes, k = [], [], 0
    for i, ((seq, target, cuts), ref, buf) in enumerate(zip(sources, in_refs, bufs)):
        rows = buf.shape[0] // cuts
        for c in range(cuts):
            part = pl.ds(c * rows, rows)
            pulls.append(pltpu.make_async_copy(ref.at[seq, part], buf.at[part], sem_in.at[k]))
            pushes.append(pltpu.make_async_copy(buf.at[part], out_refs[target].at[ids_ref[i], part], sem_out.at[k]))
            k += 1
    for pull in pulls:
        pull.start()
    for pull, push in zip(pulls, pushes):
        pull.wait()
        push.start()
    for push in pushes:
        push.wait()


def place(ids, blocks, wholes):
    n, n_copies = len(blocks), sum(cuts for *_, cuts in blocks)
    return pl.pallas_call(
        functools.partial(place_kernel, tuple(block[1:] for block in blocks), len(wholes)),
        grid_spec=pltpu.PrefetchScalarGridSpec(
            num_scalar_prefetch=1, grid=(), in_specs=[ANY] * (n + len(wholes)), out_specs=[ANY] * len(wholes),
            scratch_shapes=[pltpu.VMEM(arr.shape[1:], arr.dtype) for arr, *_ in blocks] + [pltpu.SemaphoreType.DMA((n_copies,))] * 2),
        out_shape=[jax.ShapeDtypeStruct(arr.shape, arr.dtype) for arr in wholes],
        compiler_params=pltpu.CompilerParams(vmem_limit_bytes=40 << 20),
        input_output_aliases={1 + n + i: i for i in range(len(wholes))},
        name="place",
    )(ids, *(arr for arr, *_ in blocks), *wholes)


def rope_tables(start_pos, chunk_len, key_dim):
    half_dim = key_dim // 2
    inv_freq = jnp.power(ROPE_BASE, -jnp.arange(half_dim).astype(F32) / half_dim)
    starts = (start_pos[:, None] + jnp.arange(0, chunk_len, TILE)[None, :]).astype(F32)
    base = starts[:, :, None, None] * inv_freq
    row = lax.broadcasted_iota(jnp.int32, (1, 1, 8, 1), 2)
    base = jnp.where(row == 0, jnp.cos(base), jnp.sin(base))
    step = jnp.arange(TILE).astype(F32)[None, :, None] * inv_freq
    kind = lax.broadcasted_iota(jnp.int32, (2, 1, 1), 0)
    return base.reshape(start_pos.shape[0], -1, half_dim), jnp.where(kind == 0, jnp.cos(step), jnp.sin(step))


def solution(mesh):
    n_dp = mesh.shape["dp"]

    def swap(axis, bits):
        return functools.partial(lax.ppermute, axis_name=axis, perm=[(i, i ^ bits) for i in range(mesh.shape[axis])])

    to_core, to_chip, to_far = swap("tp", 1), swap("tp", 2), swap("tp", 3)

    def local_layer(x_in, start_pos, kv_state, ln1_gain, ln1_bias, w_q, w_k, w_v, w_g, w_o, ln2_gain, ln2_bias, w_up, w_down):
        tp, group = lax.axis_index("tp"), lax.axis_index("dp")
        chip, core = tp // 2, tp % 2
        other = 1 - core
        chunk_len, d_model = x_in.shape[1:]
        own = kv_state[:, 0]
        key_dim, val_dim = own.shape[1:]

        def head_places(arrs, to=0):
            return [(w, ((to, 0, col, 0, w.shape[1], None, 0),)) for w, col in zip(arrs, (0, key_dim, 2 * key_dim, 2 * key_dim + val_dim))]

        def heads_gathered(quarters, to=0):
            return [(w, ((to, 0, 0, 0, w.shape[1], flip, 0),)) for flip, w in enumerate(quarters)]

        def mlp_places(arrs, i, to):
            at, down = i * val_dim, NUM_HEADS * val_dim
            return [(w, ((t, row, col, 0, w.shape[1], None, 0),)) for w, (t, row, col) in zip(arrs, ((to, at, 0), (to, down + at, 0), (to + 1, 0, at)))]

        def mlp_gathered(quarters, i, to):
            at, skip = i * val_dim, (NUM_HEADS - 1) * val_dim
            return [(w, ((to, at, 0, 0, d_model, flip, skip), (to + 1, 0, at, d_model, val_dim, flip, 0))) for flip, w in enumerate(quarters)]

        def mlp(to):
            return mlp_places(mlp_w, 0, to) + mlp_places(wb_core, 1, to) + mlp_gathered(wb_quarters, 2, to) + mlp_gathered(wb_far, 3, to)

        def gather(part):
            return [part] + [swap("dp", flip)(part) for flip in range(1, n_dp)]

        head_w, mlp_w = (w_q, w_k, w_v, w_g), (w_o, w_down, w_up)
        single, twice = 2 * chip + core, 4 + 2 * core
        meta = jnp.stack([single, twice, twice + 1, core, 2 * core, 2 * core + 1, group, tp, twice // 2, 2 * (1 - chip)]).astype(jnp.int32)
        wa_core = [to_core(w) for w in head_w]
        s_core = to_core(own)
        wa_part, wb_part, su_part, st_part = cut_parts(meta, head_w, mlp_w, own)
        wa_part = to_chip(wa_part)
        wb_part = to_chip(wb_part)
        su_chip = to_chip(su_part)
        st_chip = to_chip(st_part)
        wb_core = [to_core(w) for w in mlp_w]

        norms = tuple(v.reshape(1, -1) for v in (ln1_gain, ln1_bias, ln2_gain, ln2_bias))
        common = (x_in, norms, *rope_tables(start_pos, chunk_len, key_dim))
        all_seqs, pair_seqs, one = (SEQ, SEQ + 1, SEQ + 2), (SEQ + 1, SEQ + 2), (SEQ,)

        z_own_single, h_single, new_own_single = run(meta, common, one, one, (0,), (own,), head_places(head_w), n_sub=2)
        z_own_single, wa_part = lax.optimization_barrier((z_own_single, wa_part))
        wa_quarters = gather(wa_part)
        z_own, h_twice, new_states = run(meta, common, pair_seqs, pair_seqs, (0,), (own,), head_places(head_w), pair=True)
        z_own, wa_core, s_core, wb_part = lax.optimization_barrier((z_own, wa_core, s_core, wb_part))
        wb_quarters = gather(wb_part)
        hs_single, hs_twice = ((h_single, 0),), ((h_twice, 0), (h_twice, 1))
        z_core, new_core = run(meta, common, all_seqs, all_seqs, (1,), (s_core,), head_places(wa_core), hs=hs_single + hs_twice)
        z_core, wa_quarters, wb_quarters, su_chip = lax.optimization_barrier((z_core, wa_quarters, wb_quarters, su_chip))
        wa_far, wb_far, su_far = [to_core(w) for w in wa_quarters], [to_core(w) for w in wb_quarters], to_core(su_chip)
        got_core = to_core(new_core)

        z_chip, new_chip = run(meta, common, one, (STATE_SINGLE,), (2,), (su_chip,), heads_gathered(wa_quarters), n_sub=2, hs=hs_single)
        z_chip, wa_far, wb_far, wb_core, su_far, st_chip = lax.optimization_barrier((z_chip, wa_far, wb_far, wb_core, su_far, st_chip))
        st_far = to_core(st_chip)
        whole, x_single, new_far = run(meta, common, one, (STATE_SINGLE,), (3,), (su_far,), heads_gathered(wa_far) + mlp(1), ((z_own_single, 0), (z_core, 0), (z_chip, 0)), n_sub=2, hs=hs_single)
        x_single_chip = to_chip(x_single)
        x_single_core = to_core(x_single)
        got_chip = to_chip(new_chip)
        got_far = to_far(new_far)
        whole, x_a, x_b, _, _ = run(meta, common, pair_seqs, (STATE_TWICE, STATE_TWICE + 1), (2, 3), (st_chip, st_far), heads_gathered(wa_quarters) + heads_gathered(wa_far, 1) + mlp(2),
                                    ((z_own, 0), (z_core, 1)), whole, hs=hs_twice)
        x_a_core = to_core(x_a)
        x_single_far = to_core(x_single_chip)

        x_b_core = to_core(x_b)

        single_o, twice_o = 2 * chip + other, 4 + 2 * other
        far_c, far_o = 2 * (1 - chip) + core, 2 * (1 - chip) + other
        ids = jnp.stack([single_o, far_c, single, single_o, twice_o, twice_o + 1, far_c, twice_o, far_o, twice_o + 1, far_o]).astype(jnp.int32)
        cuts = chunk_len // TILE
        near = [(x_single_core, 0, 0, cuts), (x_single_chip, 0, 0, cuts)]
        near += [(arr, at, 1, 1) for arr, at in ((new_own_single, 0), (got_core, 0), (got_core, 1), (got_core, 2), (got_chip, 0))]
        whole, new_states = place(ids[:7], near, (whole, new_states))
        whole, = place(ids[7:8], [(x_a_core, 0, 0, cuts)], (whole,))
        whole, = place(ids[8:9], [(x_single_far, 0, 0, cuts)], (whole,))
        whole, new_states = place(ids[9:], [(x_b_core, 0, 0, cuts), (got_far, 0, 1, 1)], (whole, new_states))
        return whole, new_states[:, None]

    in_specs = (P("dp", None, None), P("dp"), P("dp", "tp", None, None), P(), P(), P(None, "tp"), P(None, "tp"), P(None, "tp"), P(None, "tp"), P("tp", None), P(), P(), P(None, "tp"), P("tp", None))
    out_specs = (P("dp", None, None), P("dp", "tp", None, None))
    return jax.shard_map(local_layer, mesh=mesh, in_specs=in_specs, out_specs=out_specs, check_vma=False)
```

```python
import functools

import jax
import jax.numpy as jnp
import numpy as np
from jax import lax
from jax.experimental import pallas as pl
from jax.experimental.pallas import tpu as pltpu
from jax.sharding import PartitionSpec as P


NORM_EPS = 1e-5
GROUP_EPS = 1e-6
ROPE_BASE = 10000.0
TILE = 256
NUM_HEADS = 4
LOG_GAMMA = [float(np.log1p(-np.exp2(-5.0 - n))) for n in range(NUM_HEADS)]
SEQ, STATE_SINGLE, STATE_TWICE, GROUP, HEAD, PAIR, OTHER_CHIP = 0, 3, 4, 6, 7, 8, 9
BF16 = jnp.bfloat16
F32 = jnp.float32
ANY = pl.BlockSpec(memory_space=pl.ANY)


def dot(a, b):
    return jnp.dot(a, b, preferred_element_type=F32)


def layer_norm(x_f32, norm_gain, norm_bias):
    row_mean = jnp.mean(x_f32, axis=-1, keepdims=True)
    centered = x_f32 - row_mean
    variance = jnp.mean(centered * centered, axis=-1, keepdims=True)
    return centered * lax.rsqrt(variance + NORM_EPS) * norm_gain + norm_bias


def rotate(v, cos_t, sin_t):
    half = v.shape[-1] // 2
    a, b = v[:, :half], v[:, half:]
    return jnp.concatenate([a * cos_t - b * sin_t, b * cos_t + a * sin_t], axis=-1)


def widen(row_table, width):
    return jnp.concatenate([row_table] * (width // row_table.shape[-1]), axis=-1)


def log_decay(head):
    value = jnp.float32(LOG_GAMMA[0])
    for n, log_gamma in enumerate(LOG_GAMMA[1:], 1):
        value = jnp.where(head == n, jnp.float32(log_gamma), value)
    return value


def fill_decays(log_gammas, inner_ref, rows_ref):
    gap = lax.broadcasted_iota(jnp.int32, (TILE, TILE), 0) - lax.broadcasted_iota(jnp.int32, (TILE, TILE), 1)
    row = lax.broadcasted_iota(jnp.int32, (TILE, 128), 0)
    for i, log_gamma in enumerate(log_gammas):
        inner_ref[i] = jnp.where(gap >= 0, jnp.exp(jnp.maximum(gap, 0).astype(F32) * log_gamma), 0.0)
        rows_ref[i, 0] = jnp.exp((row + 1).astype(F32) * log_gamma)
        rows_ref[i, 1] = jnp.exp((TILE - 1 - row).astype(F32) * log_gamma)
        rows_ref[i, 2] = jnp.exp(jnp.full((TILE, 128), TILE, F32) * log_gamma)


def head_blocks(hs, w_ref, state_ref, inner, rows_ref, tables):
    n_seqs, key_dim, val_dim = state_ref.shape
    out = []
    for i, (h, table) in enumerate(zip(hs, tables)):
        b = i * n_seqs // len(tables)
        q_raw = dot(h, w_ref[:, :key_dim])
        k_raw = dot(h, w_ref[:, key_dim:2 * key_dim])
        queries = rotate(q_raw, *table).astype(BF16)
        keys = (rotate(k_raw, *table) * key_dim ** -0.5).astype(BF16)
        values = dot(h, w_ref[:, 2 * key_dim:2 * key_dim + val_dim]).astype(BF16)
        scores = lax.dot_general(queries, keys, (((1,), (1,)), ((), ())), preferred_element_type=F32) * inner
        state = state_ref[b]
        carried = dot(queries, state.astype(BF16)) * widen(rows_ref[0], val_dim)
        retained = dot(scores.astype(BF16), values) + carried
        gates = dot(h, w_ref[:, 2 * key_dim + val_dim:])
        faded = (keys.astype(F32) * widen(rows_ref[1], key_dim)).astype(BF16)
        update = lax.dot_general(faded, values, (((0,), (0,)), ((), ())), preferred_element_type=F32)
        state_ref[b] = state * widen(rows_ref[2, 0:1], val_dim) + update
        row_mean = jnp.mean(retained, axis=-1, keepdims=True)
        centered = retained - row_mean
        variance = jnp.mean(centered * centered, axis=-1, keepdims=True)
        normed = centered * lax.rsqrt(variance + GROUP_EPS)
        out.append((gates * lax.logistic(gates) * normed).astype(BF16))
    return out


def kernel_body(n_seqs, n_sub, has_h, heads, n_z, pieces, with_whole, meta_ref, gain1, bias1, gain2, bias2, step_ref, *refs):
    it = iter(refs)

    def take(n):
        return [next(it) for _ in range(n)]

    x_refs, h_refs = take(n_seqs if n_z or not has_h else 0), take(n_seqs if has_h else 0)
    base_refs, s_refs, z_refs = take(n_seqs), [take(n_seqs) for _ in heads], [take(n_seqs) for _ in range(n_z)]
    sources = take(len(pieces))
    take(with_whole)
    outs = take(1 + n_seqs if n_z else 1 if has_h else 2)
    state_refs = take(len(heads))
    inner_ref, rows_ref, sem = take(3)
    weights = list(it)

    early, late, slot = [], [], 0
    for ref, cuts in zip(sources, pieces):
        for to, row, col, first, width, flip, skip in cuts:
            if flip is not None:
                quarter = meta_ref[GROUP] ^ flip
                row = pl.multiple_of(row + quarter * ref.shape[0] + quarter // 2 * skip, 256)
            dst = weights[to].at[pl.ds(row, ref.shape[0]), pl.ds(col, width)]
            (early if to < len(heads) else late).append(pltpu.make_async_copy(ref.at[:, pl.ds(first, width)], dst, sem.at[slot]))
            slot += 1

    @pl.when(pl.program_id(0) == 0)
    def _():
        for copy in early + late:
            copy.start()
        fill_decays([log_decay(meta_ref[HEAD] ^ head) for head in heads], inner_ref, rows_ref)
        for per_head, state_ref in zip(s_refs, state_refs):
            for b, s_ref in enumerate(per_head):
                state_ref[b] = s_ref[0]
        for copy in early:
            copy.wait()

    cos_b, sin_b = step_ref[0], step_ref[1]
    tables = []
    for base_ref in base_refs:
        for j in range(n_sub):
            at = pl.multiple_of((pl.program_id(0) * n_sub + j) * 8, 8)
            cos_a, sin_a = base_ref[0, pl.ds(at, 1), :], base_ref[0, pl.ds(at + 1, 1), :]
            tables.append((cos_a * cos_b - sin_a * sin_b, sin_a * cos_b + cos_a * sin_b))
    if has_h:
        normed = [h_ref[0] for h_ref in h_refs]
    else:
        normed = [layer_norm(x_ref[0].astype(F32), gain1[...], bias1[...]).astype(BF16) for x_ref in x_refs]
        for b, h in enumerate(normed):
            outs[1][b] = h
    hs = [h[j * TILE:(j + 1) * TILE] for h in normed for j in range(n_sub)]
    mixed = [head_blocks(hs, weights[i], state_refs[i], inner_ref[i], rows_ref.at[i], tables) for i in range(len(heads))]
    rows = n_sub * TILE
    if not n_z:
        for i, block in enumerate(mixed[0]):
            outs[0][i // n_sub, i % n_sub * TILE:(i % n_sub + 1) * TILE] = block
        return

    @pl.when(pl.program_id(0) == 0)
    def _():
        for copy in late:
            copy.wait()

    mixed = [[ref[0] for ref in refs_of] for refs_of in z_refs] + mixed
    w_od, w_up = weights[len(heads):]
    width = w_up.shape[1]
    u = dot(jnp.concatenate([below(z) for z in mixed], axis=1), w_od[:width])
    x_mid = (below([x_ref[0] for x_ref in x_refs]).astype(F32) + u.astype(BF16).astype(F32)).astype(BF16)
    h_two = layer_norm(x_mid.astype(F32), gain2[...], bias2[...]).astype(BF16)
    acts = []
    for at in range(0, width, width // 4):
        up = dot(h_two, w_up[:, at:at + width // 4])
        acts.append((up * 0.5 * (1.0 + lax.erf(up * 0.5 ** 0.5))).astype(BF16))
    f = dot(jnp.concatenate(acts, axis=1), w_od[width:])
    x_out = (x_mid.astype(F32) + f.astype(BF16).astype(F32)).astype(BF16)
    for b in range(n_seqs):
        outs[0][b] = x_out[b * rows:(b + 1) * rows]
        outs[1 + b][0] = x_out[b * rows:(b + 1) * rows]


def below(blocks):
    return blocks[0] if len(blocks) == 1 else jnp.concatenate(blocks, axis=0)


def run(meta, common, seqs, state_rows, heads, states, weights, zs=(), whole=None, pair=False, n_sub=1, hs=()):
    x, norms, base, step = common
    tile = n_sub * TILE
    n, chunk_len, d_model = len(seqs), x.shape[1], x.shape[2]
    key_dim, val_dim = states[0].shape[1:]

    def row_spec(shape, at):
        return pl.BlockSpec((1,) + shape, lambda t, m: (m[at], 0, 0))

    def token_spec(at):
        return pl.BlockSpec((1, tile, d_model), lambda t, m: (m[at], t, 0))

    def tile_of(width, count=1, at=0):
        return pl.BlockSpec((count, tile, width), lambda t, m: (at, t, 0))

    def resident(arr):
        return pl.BlockSpec(arr.shape, lambda t, m: (0,) * arr.ndim, pipeline_mode=pl.Buffered(1))

    specs, args = [resident(arr) for arr in (*norms, step)], [*norms, step]
    if zs or not hs:
        specs += [token_spec(at) for at in seqs]
        args += [x] * n
    specs += [tile_of(d_model, 1, at) for _, at in hs] + [row_spec(base.shape[1:], at) for at in seqs]
    args += [h for h, _ in hs] + [base] * n
    for state in states:
        specs += [row_spec(state.shape[1:], at) for at in state_rows]
        args += [state] * n
    for z, first in zs:
        specs += [tile_of(val_dim, 1, first + b) for b in range(n)]
        args += [z] * n
    pieces = [cuts for _, cuts in weights]
    args += [arr for arr, _ in weights]
    specs += [ANY] * len(weights)
    scratch = [(d_model, 2 * key_dim + 2 * val_dim)] * len(heads)
    if zs:
        scratch += [(2 * NUM_HEADS * val_dim, d_model), (d_model, NUM_HEADS * val_dim)]
    aliases = {}
    if whole is not None:
        aliases = {len(args) + 1: 0}
        args.append(whole)
        specs.append(ANY)
    if zs:
        whole_spec = token_spec(seqs[0]) if n == 1 else pl.BlockSpec((n, tile, d_model), lambda t, m: (m[PAIR], t, 0))
        outs = [(whole_spec, jax.ShapeDtypeStruct(x.shape, BF16))] + [(tile_of(d_model), jax.ShapeDtypeStruct((1, chunk_len, d_model), BF16))] * n
    else:
        outs = [(tile_of(width, n), jax.ShapeDtypeStruct((n, chunk_len, width), BF16)) for width in ((val_dim,) if hs else (val_dim, d_model))]
    state_out = pl.BlockSpec((n, key_dim, val_dim), lambda t, m: (m[PAIR] if pair else 0, 0, 0))
    outs += [(state_out, jax.ShapeDtypeStruct((x.shape[0] if pair else n, key_dim, val_dim), F32))] * len(heads)
    flops = n * len(heads) * 2 * (d_model * (2 * key_dim + 2 * val_dim) + TILE * (key_dim + val_dim) + 2 * key_dim * val_dim)
    flops += n * 24 * d_model * val_dim if zs else 0
    return pl.pallas_call(
        functools.partial(kernel_body, n, n_sub, bool(hs), tuple(heads), len(zs), tuple(pieces), whole is not None),
        grid_spec=pltpu.PrefetchScalarGridSpec(
            num_scalar_prefetch=1, grid=(chunk_len // tile,), in_specs=specs, out_specs=[spec for spec, _ in outs],
            scratch_shapes=[pltpu.VMEM((len(heads), TILE, TILE), F32), pltpu.VMEM((len(heads), 3, TILE, 128), F32), pltpu.SemaphoreType.DMA((sum(map(len, pieces)),))]
            + [pltpu.VMEM(shape, BF16) for shape in scratch]),
        out_shape=[shape for _, shape in outs],
        compiler_params=pltpu.CompilerParams(dimension_semantics=("arbitrary",), vmem_limit_bytes=62 << 20),
        cost_estimate=pl.CostEstimate(flops=chunk_len * flops, bytes_accessed=n * chunk_len * d_model * (8 if zs else 4), transcendentals=0),
        input_output_aliases=aliases,
        name="tail" if zs else "heads",
    )(meta, *args)


def parts_kernel(meta_ref, w_q, w_k, w_v, w_g, w_o, w_down, w_up, own, heads_out, mlp_out, single_out, twice_out, heads_buf, mlp_buf, single_buf, twice_buf, sem, sem_out):
    rows, group = heads_buf.shape[0], meta_ref[GROUP]
    at = pl.ds(pl.multiple_of(group * rows, rows), rows)
    half = pl.ds(pl.multiple_of((group % 2) * rows, rows), rows)
    d_model = w_o.shape[1]
    copies, col = [], 0
    for w in (w_q, w_k, w_v, w_g):
        copies.append(pltpu.make_async_copy(w.at[at], heads_buf.at[:, pl.ds(col, w.shape[1])], sem.at[len(copies)]))
        col += w.shape[1]
    copies.append(pltpu.make_async_copy(w_up.at[at], mlp_buf.at[:, pl.ds(d_model, w_up.shape[1])], sem.at[len(copies)]))
    copies.append(pltpu.make_async_copy(own.at[pl.ds(meta_ref[OTHER_CHIP], 2)], single_buf, sem.at[len(copies)]))
    copies.append(pltpu.make_async_copy(own.at[pl.ds(4, 4)], twice_buf, sem.at[len(copies)]))
    last = [pltpu.make_async_copy(w.at[half], mlp_buf.at[:, pl.ds(0, d_model)], sem.at[len(copies)]) for w in (w_o, w_down)]
    for copy in copies[:5]:
        copy.start()

    @pl.when(group < 2)
    def _():
        last[0].start()

    @pl.when(group >= 2)
    def _():
        last[1].start()

    for copy in copies[5:]:
        copy.start()
    pushes = [pltpu.make_async_copy(buf, out, sem_out.at[i]) for i, (buf, out) in
              enumerate(((heads_buf, heads_out), (mlp_buf, mlp_out), (single_buf, single_out), (twice_buf, twice_out)))]
    for push, pulls in zip(pushes, (copies[:4], [copies[4], last[0]], copies[5:6], copies[6:])):
        for pull in pulls:
            pull.wait()
        push.start()
    for push in pushes:
        push.wait()


def cut_parts(meta, head_w, mlp_w, own):
    n_rows = mlp_w[0].shape[0] // 2
    shapes = [((n_rows, sum(w.shape[1] for w in head_w)), BF16), ((n_rows, mlp_w[0].shape[1] + mlp_w[2].shape[1]), BF16), ((2,) + own.shape[1:], F32), ((4,) + own.shape[1:], F32)]
    return pl.pallas_call(
        parts_kernel,
        grid_spec=pltpu.PrefetchScalarGridSpec(num_scalar_prefetch=1, grid=(), in_specs=[ANY] * 8, out_specs=[ANY] * 4,
                                               scratch_shapes=[pltpu.VMEM(*shape) for shape in shapes] + [pltpu.SemaphoreType.DMA((8,)), pltpu.SemaphoreType.DMA((4,))]),
        out_shape=[jax.ShapeDtypeStruct(shape, dtype) for shape, dtype in shapes],
        name="parts",
    )(meta, *head_w, *mlp_w, own)


def place_kernel(sources, n_wholes, ids_ref, *refs):
    in_refs, out_refs = refs[:len(sources)], refs[len(sources) + n_wholes:len(sources) + 2 * n_wholes]
    bufs, sem_in, sem_out = refs[len(sources) + 2 * n_wholes:-2], refs[-2], refs[-1]
    pulls, pushes, k = [], [], 0
    for i, ((seq, target, cuts), ref, buf) in enumerate(zip(sources, in_refs, bufs)):
        rows = buf.shape[0] // cuts
        for c in range(cuts):
            part = pl.ds(c * rows, rows)
            pulls.append(pltpu.make_async_copy(ref.at[seq, part], buf.at[part], sem_in.at[k]))
            pushes.append(pltpu.make_async_copy(buf.at[part], out_refs[target].at[ids_ref[i], part], sem_out.at[k]))
            k += 1
    for pull in pulls:
        pull.start()
    for pull, push in zip(pulls, pushes):
        pull.wait()
        push.start()
    for push in pushes:
        push.wait()


def place(ids, blocks, wholes):
    n, n_copies = len(blocks), sum(cuts for *_, cuts in blocks)
    return pl.pallas_call(
        functools.partial(place_kernel, tuple(block[1:] for block in blocks), len(wholes)),
        grid_spec=pltpu.PrefetchScalarGridSpec(
            num_scalar_prefetch=1, grid=(), in_specs=[ANY] * (n + len(wholes)), out_specs=[ANY] * len(wholes),
            scratch_shapes=[pltpu.VMEM(arr.shape[1:], arr.dtype) for arr, *_ in blocks] + [pltpu.SemaphoreType.DMA((n_copies,))] * 2),
        out_shape=[jax.ShapeDtypeStruct(arr.shape, arr.dtype) for arr in wholes],
        compiler_params=pltpu.CompilerParams(vmem_limit_bytes=40 << 20),
        input_output_aliases={1 + n + i: i for i in range(len(wholes))},
        name="place",
    )(ids, *(arr for arr, *_ in blocks), *wholes)


def rope_tables(start_pos, chunk_len, key_dim):
    half_dim = key_dim // 2
    inv_freq = jnp.power(ROPE_BASE, -jnp.arange(half_dim).astype(F32) / half_dim)
    starts = (start_pos[:, None] + jnp.arange(0, chunk_len, TILE)[None, :]).astype(F32)
    base = starts[:, :, None, None] * inv_freq
    row = lax.broadcasted_iota(jnp.int32, (1, 1, 8, 1), 2)
    base = jnp.where(row == 0, jnp.cos(base), jnp.sin(base))
    step = jnp.arange(TILE).astype(F32)[None, :, None] * inv_freq
    kind = lax.broadcasted_iota(jnp.int32, (2, 1, 1), 0)
    return base.reshape(start_pos.shape[0], -1, half_dim), jnp.where(kind == 0, jnp.cos(step), jnp.sin(step))


def solution(mesh):
    n_dp = mesh.shape["dp"]

    def swap(axis, bits):
        return functools.partial(lax.ppermute, axis_name=axis, perm=[(i, i ^ bits) for i in range(mesh.shape[axis])])

    to_core, to_chip, to_far = swap("tp", 1), swap("tp", 2), swap("tp", 3)

    def local_layer(x_in, start_pos, kv_state, ln1_gain, ln1_bias, w_q, w_k, w_v, w_g, w_o, ln2_gain, ln2_bias, w_up, w_down):
        tp, group = lax.axis_index("tp"), lax.axis_index("dp")
        chip, core = tp // 2, tp % 2
        other = 1 - core
        chunk_len, d_model = x_in.shape[1:]
        own = kv_state[:, 0]
        key_dim, val_dim = own.shape[1:]

        def head_places(arrs, to=0):
            return [(w, ((to, 0, col, 0, w.shape[1], None, 0),)) for w, col in zip(arrs, (0, key_dim, 2 * key_dim, 2 * key_dim + val_dim))]

        def heads_gathered(quarters, to=0):
            return [(w, ((to, 0, 0, 0, w.shape[1], flip, 0),)) for flip, w in enumerate(quarters)]

        def mlp_places(arrs, i, to):
            at, down = i * val_dim, NUM_HEADS * val_dim
            return [(w, ((t, row, col, 0, w.shape[1], None, 0),)) for w, (t, row, col) in zip(arrs, ((to, at, 0), (to, down + at, 0), (to + 1, 0, at)))]

        def mlp_gathered(quarters, i, to):
            at, skip = i * val_dim, (NUM_HEADS - 1) * val_dim
            return [(w, ((to, at, 0, 0, d_model, flip, skip), (to + 1, 0, at, d_model, val_dim, flip, 0))) for flip, w in enumerate(quarters)]

        def mlp(to):
            return mlp_places(mlp_w, 0, to) + mlp_places(wb_core, 1, to) + mlp_gathered(wb_quarters, 2, to) + mlp_gathered(wb_far, 3, to)

        def gather(part):
            return [part] + [swap("dp", flip)(part) for flip in range(1, n_dp)]

        head_w, mlp_w = (w_q, w_k, w_v, w_g), (w_o, w_down, w_up)
        single, twice = 2 * chip + core, 4 + 2 * core
        meta = jnp.stack([single, twice, twice + 1, core, 2 * core, 2 * core + 1, group, tp, twice // 2, 2 * (1 - chip)]).astype(jnp.int32)
        wa_core = [to_core(w) for w in head_w]
        s_core = to_core(own)
        wa_part, wb_part, su_part, st_part = cut_parts(meta, head_w, mlp_w, own)
        wa_part = to_chip(wa_part)
        wb_part = to_chip(wb_part)
        su_chip = to_chip(su_part)
        st_chip = to_chip(st_part)
        wb_core = [to_core(w) for w in mlp_w]

        norms = tuple(v.reshape(1, -1) for v in (ln1_gain, ln1_bias, ln2_gain, ln2_bias))
        common = (x_in, norms, *rope_tables(start_pos, chunk_len, key_dim))
        all_seqs, pair_seqs, one = (SEQ, SEQ + 1, SEQ + 2), (SEQ + 1, SEQ + 2), (SEQ,)

        z_own_single, h_single, new_own_single = run(meta, common, one, one, (0,), (own,), head_places(head_w), n_sub=2)
        z_own_single, wa_part = lax.optimization_barrier((z_own_single, wa_part))
        wa_quarters = gather(wa_part)
        z_own, h_twice, new_states = run(meta, common, pair_seqs, pair_seqs, (0,), (own,), head_places(head_w), pair=True, n_sub=2)
        z_own, wa_core, s_core, wb_part = lax.optimization_barrier((z_own, wa_core, s_core, wb_part))
        wb_quarters = gather(wb_part)
        hs_single, hs_twice = ((h_single, 0),), ((h_twice, 0), (h_twice, 1))
        z_core, new_core = run(meta, common, all_seqs, all_seqs, (1,), (s_core,), head_places(wa_core), hs=hs_single + hs_twice)
        z_core, wa_quarters, wb_quarters, su_chip = lax.optimization_barrier((z_core, wa_quarters, wb_quarters, su_chip))
        wa_far, wb_far, su_far = [to_core(w) for w in wa_quarters], [to_core(w) for w in wb_quarters], to_core(su_chip)
        got_core = to_core(new_core)

        z_chip, new_chip = run(meta, common, one, (STATE_SINGLE,), (2,), (su_chip,), heads_gathered(wa_quarters), n_sub=2, hs=hs_single)
        z_chip, wa_far, wb_far, wb_core, su_far, st_chip = lax.optimization_barrier((z_chip, wa_far, wb_far, wb_core, su_far, st_chip))
        st_far = to_core(st_chip)
        whole, x_single, new_far = run(meta, common, one, (STATE_SINGLE,), (3,), (su_far,), heads_gathered(wa_far) + mlp(1), ((z_own_single, 0), (z_core, 0), (z_chip, 0)), n_sub=2, hs=hs_single)
        x_single_chip = to_chip(x_single)
        x_single_core = to_core(x_single)
        got_chip = to_chip(new_chip)
        got_far = to_far(new_far)
        whole, x_a, x_b, _, _ = run(meta, common, pair_seqs, (STATE_TWICE, STATE_TWICE + 1), (2, 3), (st_chip, st_far), heads_gathered(wa_quarters) + heads_gathered(wa_far, 1) + mlp(2),
                                    ((z_own, 0), (z_core, 1)), whole, hs=hs_twice)
        x_a_core = to_core(x_a)
        x_single_far = to_core(x_single_chip)

        x_b_core = to_core(x_b)

        single_o, twice_o = 2 * chip + other, 4 + 2 * other
        far_c, far_o = 2 * (1 - chip) + core, 2 * (1 - chip) + other
        ids = jnp.stack([single_o, far_c, single, single_o, twice_o, twice_o + 1, far_c, twice_o, far_o, twice_o + 1, far_o]).astype(jnp.int32)
        cuts = chunk_len // TILE
        near = [(x_single_core, 0, 0, cuts), (x_single_chip, 0, 0, cuts)]
        near += [(arr, at, 1, 1) for arr, at in ((new_own_single, 0), (got_core, 0), (got_core, 1), (got_core, 2), (got_chip, 0))]
        whole, new_states = place(ids[:7], near, (whole, new_states))
        whole, = place(ids[7:8], [(x_a_core, 0, 0, cuts)], (whole,))
        whole, = place(ids[8:9], [(x_single_far, 0, 0, cuts)], (whole,))
        whole, new_states = place(ids[9:], [(x_b_core, 0, 0, cuts), (got_far, 0, 1, 1)], (whole, new_states))
        return whole, new_states[:, None]

    in_specs = (P("dp", None, None), P("dp"), P("dp", "tp", None, None), P(), P(), P(None, "tp"), P(None, "tp"), P(None, "tp"), P(None, "tp"), P("tp", None), P(), P(), P(None, "tp"), P("tp", None))
    out_specs = (P("dp", None, None), P("dp", "tp", None, None))
    return jax.shard_map(local_layer, mesh=mesh, in_specs=in_specs, out_specs=out_specs, check_vma=False)
```
